32 devices in a mesh: row: 16 (over z, y, x), col: 2 (over core).
Axes of the slice: x: 2, y: 2, z: 4, core: 2. Of those that a mesh axis runs over, the one named last changes fastest.
Arguments:
- incident: bfloat16 [2, 8192, 512], P(None, ('row', 'col')), may hold values from -6 to 6
- near_tiles: bfloat16 [32, 2, 3, 2, 256, 256], P(('row', 'col')), may hold values from -0.15625 to 0.15625
- near_offsets: int32 [32, 3], P(('row', 'col')), may hold values from -2 to 2, as said below
- far_row: int32 [16, 2, 16], P('row', 'col'), may hold values from 0 to 1, as said below
- far_col: int32 [16, 2, 16], P('row', 'col'), may hold values from 0 to 15
- far_rank: int32 [16, 2, 16], P('row', 'col'), may hold values from 8 to 32, as said below
- far_count: int32 [16, 2], P('row', 'col'), may hold values from 2 to 16, as said below
- far_u: bfloat16 [16, 2, 2, 16, 2, 32, 256], P('row', 'col'), may hold values from -0.25 to 0.25
- far_v: bfloat16 [16, 2, 2, 16, 2, 32, 256], P('row', 'col'), may hold values from -0.25 to 0.25
Outputs:
- response: bfloat16 [2, 8192, 512], P(None, ('row', 'col'))
The draws below stay inside these ranges and needn't reach their ends.
Inputs may be any that keep to these rules, and one draw needn't show every extreme that they name: `near_offsets`: slot 0 of every tile is 0; the other slots of a tile hold distinct values among -2, -1, 1, 2. On one device the pairs (far_row, far_col) of all 16 slots are distinct, and every block (i, j) they name has circular tile distance 3 or more between i and j. `far_rank`: slot 0 of every device has rank 32. `far_count`: some device has all 16 slots live.
All inputs are finite; a program needn't handle non-finite values.
Results may differ from the reference program's by a relative error of at most 0.0035.
Values may be sent and summed in bfloat16 or wider, within the bound.
A program may use at most 192 MiB of HBM per device.

```python
import jax
import jax.numpy as jnp
from jax import lax

TILE = 256
RANK = 32
NEAR_SLOTS = 3
WAVES = 2
SOURCES = 256
FAR_SLOTS = 16
TILES = 32
PANELS = 8192
N_ROW = 16
N_COL = 2


def draw_near_offsets(key, part):
    tile_count = N_ROW * N_COL
    scores = jax.random.randint(jax.random.fold_in(key, 11), (tile_count, 4), 0, 1 << 20) * 4 + jnp.arange(4, dtype=jnp.int32)[None, :]
    ranking = jnp.argsort(scores, axis=1)
    offset_table = jnp.array([-2, -1, 1, 2], dtype=jnp.int32)
    picked = offset_table[ranking[:, :NEAR_SLOTS - 1]]
    return jnp.concatenate([jnp.zeros((tile_count, 1), jnp.int32), picked], axis=1).astype(jnp.int32)


def far_layout(key):
    pair_count = N_COL * N_ROW
    tile_count = N_ROW * N_COL
    pair_ids = jnp.arange(pair_count, dtype=jnp.int32)
    local_row = pair_ids // N_ROW
    col_device = pair_ids % N_ROW
    row_index = jnp.arange(N_ROW, dtype=jnp.int32)[:, None, None]
    col_index = jnp.arange(N_COL, dtype=jnp.int32)[None, :, None]
    row_tile = row_index * N_COL + local_row[None, None, :]
    col_tile = col_device[None, None, :] * N_COL + col_index
    forward_gap = (row_tile - col_tile) % tile_count
    circular = jnp.minimum(forward_gap, tile_count - forward_gap)
    random_part = jax.random.randint(jax.random.fold_in(key, 21), (N_ROW, N_COL, pair_count), 0, 1 << 19)
    scores = random_part * 1024 + pair_ids[None, None, :] + jnp.where(circular < 3, 1 << 30, 0)
    ranking = jnp.argsort(scores, axis=2)[:, :, :FAR_SLOTS]
    return ((ranking // N_ROW).astype(jnp.int32), (ranking % N_ROW).astype(jnp.int32))


def draw_far_row(key, part):
    return far_layout(key)[0]


def draw_far_col(key, part):
    return far_layout(key)[1]


def draw_far_rank(key, part):
    sampled = jax.random.randint(jax.random.fold_in(key, 31), (N_ROW, N_COL, FAR_SLOTS), max(1, RANK // 4), RANK + 1)
    leading = (jnp.arange(FAR_SLOTS, dtype=jnp.int32) == 0)[None, None, :]
    return jnp.where(leading, RANK, sampled).astype(jnp.int32)


def draw_far_count(key, part):
    lowest = max(1, FAR_SLOTS // 8)
    spread = FAR_SLOTS - lowest
    uniform_part = jax.random.randint(jax.random.fold_in(key, 41), (N_ROW, N_COL), 0, spread + 1)
    counts = lowest + uniform_part * uniform_part // spread
    fullest = jax.random.randint(jax.random.fold_in(key, 42), (), 0, N_ROW * N_COL)
    flat_index = jnp.arange(N_ROW * N_COL, dtype=jnp.int32).reshape(N_ROW, N_COL)
    return jnp.where(flat_index == fullest, FAR_SLOTS, counts).astype(jnp.int32)


def levels(rng, extent, pieces, least, high):
    def one(position, parts):
        draws = jax.random.uniform(jax.random.fold_in(jax.random.fold_in(rng, 6), position), (parts,), jnp.float32, least / len(pieces), high / len(pieces))
        return jnp.repeat(jnp.exp(draws), extent[position] // parts).reshape((-1,) + (1,) * (len(extent) - position - 1))

    loudness = one(*pieces[0])
    for cut in pieces[1:]:
        loudness = loudness * one(*cut)
    return loudness


def normal_values(own_key, extent, width, most, pieces=(), held_as=jnp.bfloat16):
    level = levels(own_key, extent, pieces, -0.22, 0.18) if pieces else 1.0
    drawn = jax.random.normal(own_key, extent, jnp.float32) * width * level
    return jnp.minimum(jnp.maximum(drawn, -most), most).astype(held_as)


def setup_inputs(seed: int = 0) -> dict:
    keys = jax.random.split(jax.random.key(seed), 10)
    return {
        "incident": normal_values(keys[0], (WAVES, PANELS, 2 * SOURCES), 1.0, 6.0, ((1, 32),)),
        "near_tiles": normal_values(keys[1], (TILES, WAVES, NEAR_SLOTS, 2, TILE, TILE), (2 * TILE * NEAR_SLOTS) ** -0.5, 0.15625, ((0, 32),)),
        "near_offsets": draw_near_offsets(jax.random.fold_in(keys[9], 71), 0),
        "far_row": draw_far_row(jax.random.fold_in(keys[9], 71), 0),
        "far_col": draw_far_col(jax.random.fold_in(keys[9], 71), 0),
        "far_rank": draw_far_rank(jax.random.fold_in(keys[9], 71), 0),
        "far_count": draw_far_count(jax.random.fold_in(keys[9], 71), 0),
        "far_u": normal_values(keys[7], (N_ROW, N_COL, WAVES, FAR_SLOTS, 2, RANK, TILE), (RANK * FAR_SLOTS) ** -0.5, 0.25, ((0, 16), (1, 2))),
        "far_v": normal_values(keys[8], (N_ROW, N_COL, WAVES, FAR_SLOTS, 2, RANK, TILE), (2 * TILE) ** -0.5, 0.25, ((0, 16), (1, 2))),
    }


def combine_parts(real_prod, imag_prod):
    half_width = real_prod.shape[-1] // 2
    return jnp.concatenate([real_prod[..., :half_width] - imag_prod[..., half_width:], real_prod[..., half_width:] + imag_prod[..., :half_width]], axis=-1)


def reference(incident, near_tiles, near_offsets, far_row, far_col, far_rank, far_count, far_u, far_v):
    tile_count = N_ROW * N_COL
    columns = incident.shape[-1]
    tiles_input = incident.reshape(WAVES, tile_count, TILE, columns)
    near_groups = near_tiles.reshape(N_ROW, N_COL, WAVES, NEAR_SLOTS, 2, TILE, TILE)
    offset_groups = near_offsets.reshape(N_ROW, N_COL, NEAR_SLOTS)
    slot_ids = jnp.arange(FAR_SLOTS, dtype=jnp.int32)
    rank_ids = jnp.arange(RANK, dtype=jnp.int32)
    block_ids = jnp.arange(N_COL, dtype=jnp.int32)

    def one_group(packed):
        group_index, near_part, offset_part, rows_part, cols_part, rank_part, count_part, u_part, v_part = packed
        own_tiles = group_index * N_COL + block_ids
        near_index = ((own_tiles[:, None] + offset_part) % tile_count).astype(jnp.int32)
        near_inputs = tiles_input[:, near_index].astype(jnp.float32)
        near_float = near_part.astype(jnp.float32)
        real_prod = jnp.einsum("awnpq,wanqc->wapc", near_float[:, :, :, 0], near_inputs)
        imag_prod = jnp.einsum("awnpq,wanqc->wapc", near_float[:, :, :, 1], near_inputs)
        result_rows = combine_parts(real_prod, imag_prod)
        for col_group in range(N_COL):
            col_tiles = (cols_part[col_group] * N_COL + col_group).astype(jnp.int32)
            live_mask = ((slot_ids < count_part[col_group])[:, None] & (rank_ids[None, :] < rank_part[col_group][:, None])).astype(jnp.float32)
            select = (rows_part[col_group][:, None] == block_ids[None, :]).astype(jnp.float32)
            for wave_index in range(WAVES):
                slot_tiles = tiles_input[wave_index, col_tiles].astype(jnp.float32)
                v_factor = v_part[col_group, wave_index].astype(jnp.float32)
                coefficients = combine_parts(jnp.einsum("fkq,fqc->fkc", v_factor[:, 0], slot_tiles), jnp.einsum("fkq,fqc->fkc", v_factor[:, 1], slot_tiles))
                coefficients = lax.optimization_barrier((coefficients * live_mask[:, :, None]).astype(jnp.bfloat16)).astype(jnp.float32)
                u_factor = u_part[col_group, wave_index].astype(jnp.float32)
                contrib = combine_parts(jnp.einsum("fkp,fkc->fpc", u_factor[:, 0], coefficients), jnp.einsum("fkp,fkc->fpc", u_factor[:, 1], coefficients))
                added = jnp.einsum("fa,fpc->apc", select, contrib, precision=lax.Precision.HIGHEST)
                result_rows = result_rows.at[wave_index].add(added)
        return result_rows.astype(jnp.bfloat16)

    grouped = lax.map(one_group, (jnp.arange(N_ROW, dtype=jnp.int32), near_groups, offset_groups, far_row, far_col, far_rank, far_count, far_u, far_v))
    return jnp.transpose(grouped, (1, 0, 2, 3, 4)).reshape(WAVES, tile_count * TILE, columns)
```

```python
import functools

import jax
import jax.numpy as jnp
from jax import lax
from jax.experimental import pallas as pl
from jax.experimental.pallas import tpu as pltpu
from jax.sharding import PartitionSpec as P

MESH = pl.DeviceIdType.MESH
UP, DOWN, ALONG_Y, ALONG_X = range(4)


def from_behind(value, axis, steps):
    count = lax.axis_size(axis)
    pairs = [(source, (source + steps) % count) for source in range(count)]
    return lax.ppermute(value, axis, pairs)


def combine_parts(real_prod, imag_prod):
    half_width = real_prod.shape[-1] // 2
    return jnp.concatenate(
        [
            real_prod[..., :half_width] - imag_prod[..., half_width:],
            real_prod[..., half_width:] + imag_prod[..., :half_width],
        ],
        axis=-1,
    )


def far_partial(
    wave_tiles,
    rows_local,
    cols_local,
    rank_local,
    live_count,
    u_wave,
    v_wave,
    group_limit,
    row_blocks,
):
    group_size = 16
    tile_rows = wave_tiles.shape[1]
    columns = wave_tiles.shape[2]
    rank_size = v_wave.shape[2]
    slot_ids = jnp.arange(group_size, dtype=jnp.int32)
    rank_ids = jnp.arange(rank_size, dtype=jnp.int32)

    def add_group(group_step, far_sum):
        first_slot = group_step * group_size
        rows_group = lax.dynamic_slice_in_dim(rows_local, first_slot, group_size)
        cols_group = lax.dynamic_slice_in_dim(cols_local, first_slot, group_size)
        rank_group = lax.dynamic_slice_in_dim(rank_local, first_slot, group_size)
        v_group = lax.dynamic_slice_in_dim(v_wave, first_slot, group_size, 0)
        u_group = lax.dynamic_slice_in_dim(u_wave, first_slot, group_size, 0)
        slot_tiles = jnp.take(wave_tiles, cols_group, axis=0)
        real_prod = jnp.einsum(
            "fkq,fqc->fkc", v_group[:, 0], slot_tiles, preferred_element_type=jnp.float32
        )
        imag_prod = jnp.einsum(
            "fkq,fqc->fkc", v_group[:, 1], slot_tiles, preferred_element_type=jnp.float32
        )
        live_mask = (first_slot + slot_ids < live_count)[:, None] & (
            rank_ids[None, :] < rank_group[:, None]
        )
        coefficients = (
            combine_parts(real_prod, imag_prod) * live_mask[:, :, None].astype(jnp.float32)
        ).astype(jnp.bfloat16)
        real_back = jnp.einsum(
            "fkp,fkc->fpc", u_group[:, 0], coefficients, preferred_element_type=jnp.float32
        )
        imag_back = jnp.einsum(
            "fkp,fkc->fpc", u_group[:, 1], coefficients, preferred_element_type=jnp.float32
        )
        contrib = combine_parts(real_back, imag_back)
        return far_sum.at[rows_group].add(contrib)

    zero_sum = jnp.zeros((row_blocks, tile_rows, columns), jnp.float32)
    return lax.fori_loop(0, group_limit, add_group, zero_sum)


def reduce_rows(far_sum, row_blocks, tile_rows, columns):
    flat_rows = far_sum.reshape(row_blocks * tile_rows, columns)
    return lax.psum_scatter(flat_rows, "col", scatter_dimension=0, tiled=True)


def generic_shards(incident, near_tiles, near_offsets, far_row, far_col, far_rank, far_count, far_u, far_v):
    wave_count, tile_rows, columns = incident.shape
    row_blocks = lax.axis_size("col")
    slot_count = far_row.shape[2]
    stacked = []
    for shift_by in (2, 1, 0, -1, -2):
        if shift_by == 0:
            stacked.append(incident)
        else:
            stacked.append(from_behind(incident, ("row", "col"), shift_by))
    neighbour = jnp.stack(stacked, axis=1)
    near_inputs = jnp.take(neighbour, near_offsets[0] + 2, axis=1)
    local_near = near_tiles[0]
    real_prod = jnp.einsum(
        "wnpq,wnqc->wpc", local_near[:, :, 0], near_inputs, preferred_element_type=jnp.float32
    )
    imag_prod = jnp.einsum(
        "wnpq,wnqc->wpc", local_near[:, :, 1], near_inputs, preferred_element_type=jnp.float32
    )
    near_total = combine_parts(real_prod, imag_prod)
    rows_local = far_row[0, 0]
    cols_local = far_col[0, 0]
    rank_local = far_rank[0, 0]
    live_count = far_count[0, 0]
    group_limit = slot_count // 16
    gathered = lax.all_gather(incident, "row", axis=1, tiled=True)
    outputs = []
    for wave_index in range(wave_count):
        wave_columns = gathered[wave_index]
        wave_tiles = wave_columns.reshape(-1, tile_rows, columns)
        far_sum = far_partial(
            wave_tiles,
            rows_local,
            cols_local,
            rank_local,
            live_count,
            far_u[0, 0, wave_index],
            far_v[0, 0, wave_index],
            group_limit,
            row_blocks,
        )
        own_rows = reduce_rows(far_sum, row_blocks, tile_rows, columns)
        outputs.append(near_total[wave_index] + own_rows)
    return jnp.stack(outputs, axis=0).astype(jnp.bfloat16)


def fused_kernel(
    depth, offset_ref, row_ref, col_ref, rank_ref, count_ref, x_hbm, near_hbm, u_hbm, v_hbm, out_ref,
    tiles, near_buf, u_buf, v_buf, u_turn, u_give, coef, give, v_out, v_in, served, total, keys, table,
    recv_sem, send_sem, pair_sem, v_send, v_recv, s_send, s_recv, g_send, g_recv, t_send, t_recv, load_sem,
):
    waves = tiles.shape[0]
    row_count = depth * 4
    places = depth * 2
    half = depth // 2
    row_blocks = table.shape[1]
    slots = v_buf.shape[1]
    rank_rows = v_buf.shape[3]
    tile_rows = tiles.shape[2]
    r = lax.axis_index("row")
    c = lax.axis_index("col")
    z, y, x = r // 4, (r // 2) % 2, r % 2
    own_slot, edge_slot = row_count, row_count + 1
    edge_tile = (r + 1 - 2 * c + row_count) % row_count
    side = 2 * x - 1
    partner = r + 2 * (1 - 2 * y)
    corner = (r + side + row_count) % row_count
    partner_corner = (partner + side + row_count) % row_count
    has_up, has_down = z < depth - 1, z > 0

    def row_of(tz, ty, tx):
        return (tz * 2 + ty) * 2 + tx

    load_x = [
        pltpu.make_async_copy(x_hbm.at[wave], tiles.at[wave, r], load_sem.at[3 + wave])
        for wave in range(waves)
    ]
    load_v = pltpu.make_async_copy(v_hbm.at[0, 0], v_buf, load_sem.at[0])
    load_u = pltpu.make_async_copy(u_hbm.at[0, 0], u_buf, load_sem.at[1])
    load_near = pltpu.make_async_copy(near_hbm.at[0], near_buf, load_sem.at[2])
    for load in load_x + [load_v, load_u, load_near]:
        load.start()

    barrier = pltpu.get_barrier_semaphore()

    def greet(device):
        pl.semaphore_signal(barrier, inc=1, device_id=device, device_id_type=MESH)

    for device in ((partner, c), (partner, 1 - c), (row_of(z, y, 1 - x), c), (r, 1 - c)):
        greet(device)

    @pl.when(has_up)
    def _():
        greet((row_of(z + 1, y, x), c))

    @pl.when(has_down)
    def _():
        greet((row_of(z - 1, y, x), c))

    for s in range(slots):
        key = row_ref[0, 0, s] * row_count + col_ref[0, 0, s]
        keys[s] = jnp.where(s < count_ref[0, 0], key, -1)

    def look_up(a, tile):
        wanted = a * row_count + tile
        slot, rank = jnp.int32(0), jnp.int32(0)
        for s in range(slots):
            hit = keys[s] == wanted
            slot = jnp.where(hit, s, slot)
            rank = jnp.where(hit, rank_ref[0, 0, s], rank)
        table[0, a, tile] = slot
        table[1, a, tile] = rank

    pl.semaphore_wait(barrier, 4 + jnp.where(has_up, 1, 0) + jnp.where(has_down, 1, 0))

    def copy_to(source, target, sent, received, device):
        return pltpu.make_async_remote_copy(
            src_ref=source,
            dst_ref=target,
            send_sem=sent,
            recv_sem=received,
            device_id=device,
            device_id_type=MESH,
        )

    def hop(wave, tile, link, row):
        here = tiles.at[wave, tile]
        return copy_to(here, here, send_sem.at[wave, tile, link], recv_sem.at[wave, tile], (row, c))

    def along_z(wave, tile, step):
        return hop(wave, tile, (1 - step) // 2, row_of(z + step, y, x))

    def along_x(wave, tile):
        return hop(wave, tile, ALONG_X, row_of(z, y, 1 - x))

    def along_y(wave, tile):
        return hop(wave, tile, ALONG_Y, partner)

    def to_pair(wave, tile, slot):
        return copy_to(
            tiles.at[wave, tile],
            tiles.at[wave, slot],
            pair_sem.at[wave, slot - row_count],
            recv_sem.at[wave, slot],
            (r, 1 - c),
        )

    def coef_at(plane, place, side_of):
        return coef.at[plane * half + place // 4, :, side_of, place % 4]

    def send_v(place):
        return copy_to(
            v_out.at[place], v_in.at[place], v_send.at[place], v_recv.at[place], (partner, c)
        )

    def send_served(place, j):
        return copy_to(
            served.at[place, j],
            coef_at(1, place, j),
            s_send.at[place, j],
            s_recv.at[place, j],
            (partner, c if j == 0 else 1 - c),
        )

    def send_give(plane, place, index):
        return copy_to(
            give.at[index],
            coef_at(plane, place, 1),
            g_send.at[index],
            g_recv.at[index],
            (r, 1 - c),
        )

    def send_turn(chunk):
        return copy_to(
            u_give.at[chunk],
            u_turn.at[chunk, :, :, pl.ds(4 * rank_rows, 4 * rank_rows)],
            t_send.at[chunk],
            t_recv.at[chunk],
            (r, 1 - c),
        )

    middle = jnp.minimum(z, depth - 1 - z)

    def level_of(step):
        reach = (step + 1) // 2
        near_level = z + jnp.where(step % 2 == 1, reach, -reach)
        beyond = step - middle
        far_level = z + jnp.where(depth - 1 - z > z, beyond, -beyond)
        return jnp.where(step <= 2 * middle, near_level, far_level)

    def tile_at(plane, place):
        level, other = level_of(place // 2), place % 2
        return row_of(level, y + plane - 2 * y * plane, x + other - 2 * x * other)

    def complex_rows(prod, at):
        at = 2 * rank_rows * at
        return combine_parts(prod[at:at + rank_rows], prod[at + rank_rows:at + 2 * rank_rows])

    def project(plane, place, tile, index):
        chunk, at = plane * half + place // 4, place % 4
        for wave in range(waves):
            factors = [
                v_buf[wave, table[0, a, tile]].reshape(2 * rank_rows, -1) for a in (c, 1 - c)
            ]
            prod = jnp.dot(
                jnp.concatenate(factors, axis=0),
                tiles[wave, tile],
                preferred_element_type=jnp.float32,
            )
            coef[chunk, wave, 0, at] = complex_rows(prod, 0).astype(jnp.bfloat16)
            give[index, wave] = complex_rows(prod, 1).astype(jnp.bfloat16)
        send_give(plane, place, index).start()

    def serve(place, tile):
        for wave in range(waves):
            left = v_in[place, wave].reshape(row_blocks * 2 * rank_rows, -1)
            prod = jnp.dot(left, tiles[wave, tile], preferred_element_type=jnp.float32)
            for j in range(row_blocks):
                served[place, j, wave] = complex_rows(prod, j).astype(jnp.bfloat16)
        for j in range(row_blocks):
            send_served(place, j).start()

    def arrive(wave, tile):
        pltpu.make_async_copy(tiles.at[wave, tile], tiles.at[wave, tile], recv_sem.at[wave, tile]).wait()

    def share_edge(wave, tile):
        @pl.when(tile == edge_tile)
        def _():
            to_pair(wave, tile, edge_slot).start()

    for wave in range(waves):
        load_x[wave].wait()
        along_x(wave, r).start()

        @pl.when(has_up)
        def _():
            along_z(wave, r, 1).start()

        @pl.when(has_down)
        def _():
            along_z(wave, r, -1).start()

        to_pair(wave, r, own_slot).start()

    load_v.wait()

    def push_v(place, carry):
        tile = tile_at(1, place)
        for a in range(row_blocks):
            look_up(a, tile)

        @pl.when(tile != corner)
        def _():
            for wave in range(waves):
                for j, a in enumerate((c, 1 - c)):
                    v_out[place, wave, j] = v_buf[wave, table[0, a, tile]]
            send_v(place).start()

        return carry

    lax.fori_loop(0, places, push_v, 0)

    def find_own(place, carry):
        for a in range(row_blocks):
            look_up(a, tile_at(0, place))
        return carry

    lax.fori_loop(0, places, find_own, 0)
    load_u.wait()
    load_near.wait()
    rank_ids = lax.broadcasted_iota(jnp.int32, (rank_rows, tile_rows), 0)

    def place_u(chunk):
        plane, first = chunk // half, (chunk % half) * 4
        for wave in range(waves):
            for j, a in enumerate((c, 1 - c)):
                for part in range(2):
                    rows = []
                    for at in range(4):
                        tile = tile_at(plane, first + at)
                        factor = u_buf[wave, table[0, a, tile], part].astype(jnp.float32)
                        rows.append(jnp.where(rank_ids < table[1, a, tile], factor, 0.0))
                    flipped = jnp.concatenate(rows, axis=0).T.astype(jnp.bfloat16)
                    lines = pl.ds(part * tile_rows, tile_rows)
                    if j == 0:
                        u_turn[chunk, wave, lines, 0:4 * rank_rows] = flipped
                    else:
                        u_give[chunk, wave, lines, :] = flipped
        send_turn(chunk).start()

    def use_tile(place, chunk=None):
        tile = tile_at(0, place)
        project(0, place, tile, place)
        if chunk is not None:
            place_u(chunk)

        @pl.when(tile != partner_corner)
        def _():
            send_v(place).wait_recv()
            serve(place, tile)

    def spread(step, carry):
        @pl.when(step < depth)
        def _():
            level = level_of(step)
            tile = row_of(level, y, x)

            @pl.when(step > 0)
            def _():
                for wave in range(waves):
                    arrive(wave, tile)

                    @pl.when((level < z) & has_up)
                    def _():
                        along_z(wave, tile, 1).start()

                    @pl.when((level > z) & has_down)
                    def _():
                        along_z(wave, tile, -1).start()

                    along_x(wave, tile).start()

            use_tile(2 * step, step)

        @pl.when(step >= 1)
        def _():
            place = 2 * step - 1
            tile = tile_at(0, place)
            for wave in range(waves):
                arrive(wave, tile)
                share_edge(wave, tile)

                @pl.when(tile == partner_corner)
                def _():
                    along_y(wave, tile).start()

            use_tile(place)

        return carry

    lax.fori_loop(0, depth + 1, spread, 0)

    corner_place = 1
    for step in range(depth):
        corner_place += jnp.where(row_of(level_of(step), 1 - y, 1 - x) == corner, 2 * step, 0)
    for wave in range(waves):
        arrive(wave, corner)
        share_edge(wave, corner)
    project(1, corner_place, corner, places)

    def far_chunk(chunk, wave):
        right = coef[chunk, wave].reshape(-1, coef.shape[-1])
        return jnp.dot(u_turn[chunk, wave], right, preferred_element_type=jnp.float32)

    for wave in range(waves):
        arrive(wave, own_slot)
        arrive(wave, edge_slot)
    for chunk in range(half):
        send_turn(chunk).wait_recv()
    for place in range(places):
        send_give(0, place, place).wait_recv()

    def place_of(offset):
        even = (r + offset // 2 + row_count) % row_count
        same_chip = offset == 1 - 2 * c
        return jnp.where(offset % 2 == 0, even, jnp.where(same_chip, own_slot, edge_slot))

    def first_sum(wave, carry):
        value = far_chunk(0, wave)
        for chunk in range(1, half):
            value += far_chunk(chunk, wave)
        for n in range(near_buf.shape[1]):
            left = near_buf[wave, n].reshape(2 * tile_rows, tile_rows)
            block = tiles[wave, place_of(offset_ref[0, n])]
            value += jnp.dot(left, block, preferred_element_type=jnp.float32)
        total[wave] = value
        return carry

    lax.fori_loop(0, waves, first_sum, 0)

    for chunk in range(half):
        send_turn(half + chunk).wait_recv()
        for place in range(4 * chunk, 4 * chunk + 4):
            tile = tile_at(1, place)

            @pl.when(tile != corner)
            def _():
                for j in range(row_blocks):
                    send_served(place, j).wait_recv()

            @pl.when(tile == corner)
            def _():
                send_give(1, place, places).wait_recv()

        for wave in range(waves):
            value = total[wave] + far_chunk(half + chunk, wave)
            if chunk < half - 1:
                total[wave] = value
            else:
                out_ref[wave] = combine_parts(value[:tile_rows], value[tile_rows:]).astype(out_ref.dtype)

    for wave in range(waves):
        to_pair(wave, r, own_slot).wait_send()
        to_pair(wave, edge_tile, edge_slot).wait_send()
        along_y(wave, partner_corner).wait_send()
    send_give(1, corner_place, places).wait_send()

    def drain(step, carry):
        level = level_of(step)
        tile = row_of(level, y, x)
        send_turn(step).wait_send()
        for wave in range(waves):
            along_x(wave, tile).wait_send()

            @pl.when((level <= z) & has_up)
            def _():
                along_z(wave, tile, 1).wait_send()

            @pl.when((level >= z) & has_down)
            def _():
                along_z(wave, tile, -1).wait_send()

        for other in range(2):
            place = 2 * step + other
            send_give(0, place, place).wait_send()

            @pl.when(tile_at(1, place) != corner)
            def _():
                send_v(place).wait_send()

            @pl.when(tile_at(0, place) != partner_corner)
            def _():
                for j in range(row_blocks):
                    send_served(place, j).wait_send()

        return carry

    lax.fori_loop(0, depth, drain, 0)


def fused_shards(incident, near_tiles, near_offsets, far_row, far_col, far_rank, far_count, far_u, far_v):
    waves, tile_rows, columns = incident.shape
    row_count, row_blocks = lax.axis_size("row"), lax.axis_size("col")
    slots, rank_rows = far_u.shape[3], far_u.shape[5]
    near_slots = near_tiles.shape[2]
    depth, places = row_count // 4, row_count // 2
    bf16, f32 = jnp.bfloat16, jnp.float32
    any_space = pl.BlockSpec(memory_space=pl.ANY)
    smem = pl.BlockSpec(memory_space=pltpu.SMEM)
    vmem = pl.BlockSpec(memory_space=pltpu.VMEM)
    dma = pltpu.SemaphoreType.DMA
    return pl.pallas_call(
        functools.partial(fused_kernel, depth),
        out_shape=jax.ShapeDtypeStruct(incident.shape, bf16),
        in_specs=[smem] * 5 + [any_space] * 4,
        out_specs=vmem,
        scratch_shapes=[
            pltpu.VMEM((waves, row_count + 2, tile_rows, columns), bf16),
            pltpu.VMEM((waves, near_slots, 2, tile_rows, tile_rows), bf16),
            pltpu.VMEM((waves, slots, 2, rank_rows, tile_rows), bf16),
            pltpu.VMEM((waves, slots, 2, rank_rows, tile_rows), bf16),
            pltpu.VMEM((depth, waves, 2 * tile_rows, 8 * rank_rows), bf16),
            pltpu.VMEM((depth, waves, 2 * tile_rows, 4 * rank_rows), bf16),
            pltpu.VMEM((depth, waves, row_blocks, 4, rank_rows, columns), bf16),
            pltpu.VMEM((places + 1, waves, rank_rows, columns), bf16),
            pltpu.VMEM((places, waves, row_blocks, 2, rank_rows, tile_rows), bf16),
            pltpu.VMEM((places, waves, row_blocks, 2, rank_rows, tile_rows), bf16),
            pltpu.VMEM((places, row_blocks, waves, rank_rows, columns), bf16),
            pltpu.VMEM((waves, 2 * tile_rows, columns), f32),
            pltpu.SMEM((slots,), jnp.int32),
            pltpu.SMEM((2, row_blocks, row_count), jnp.int32),
            dma((waves, row_count + 2)),
            dma((waves, row_count, 4)),
            dma((waves, 2)),
            dma((places,)),
            dma((places,)),
            dma((places, row_blocks)),
            dma((places, row_blocks)),
            dma((places + 1,)),
            dma((places + 1,)),
            dma((depth,)),
            dma((depth,)),
            dma((3 + waves,)),
        ],
        compiler_params=pltpu.CompilerParams(collective_id=0, has_side_effects=True),
    )(near_offsets, far_row, far_col, far_rank, far_count, incident, near_tiles, far_u, far_v)


def solution(mesh):
    in_specs = (
        P(None, ("row", "col"), None),
        P(("row", "col"), None, None, None, None, None),
        P(("row", "col"), None),
        P("row", "col", None),
        P("row", "col", None),
        P("row", "col", None),
        P("row", "col"),
        P("row", "col", None, None, None, None, None),
        P("row", "col", None, None, None, None, None),
    )
    out_specs = P(None, ("row", "col"), None)
    paired = mesh.shape["col"] == 2 and mesh.shape["row"] % 8 == 0
    shards = fused_shards if paired else generic_shards
    return jax.shard_map(shards, mesh=mesh, in_specs=in_specs, out_specs=out_specs, check_vma=False)
```

```python
import functools

import jax
import jax.numpy as jnp
from jax import lax
from jax.experimental import pallas as pl
from jax.experimental.pallas import tpu as pltpu
from jax.sharding import PartitionSpec as P

MESH = pl.DeviceIdType.MESH
SIDE_FROM = 0
UP, DOWN, ALONG_Y, ALONG_X = range(4)


def from_behind(value, axis, steps):
    count = lax.axis_size(axis)
    pairs = [(source, (source + steps) % count) for source in range(count)]
    return lax.ppermute(value, axis, pairs)


def combine_parts(real_prod, imag_prod):
    half_width = real_prod.shape[-1] // 2
    return jnp.concatenate(
        [
            real_prod[..., :half_width] - imag_prod[..., half_width:],
            real_prod[..., half_width:] + imag_prod[..., :half_width],
        ],
        axis=-1,
    )


def far_partial(
    wave_tiles,
    rows_local,
    cols_local,
    rank_local,
    live_count,
    u_wave,
    v_wave,
    group_limit,
    row_blocks,
):
    group_size = 16
    tile_rows = wave_tiles.shape[1]
    columns = wave_tiles.shape[2]
    rank_size = v_wave.shape[2]
    slot_ids = jnp.arange(group_size, dtype=jnp.int32)
    rank_ids = jnp.arange(rank_size, dtype=jnp.int32)

    def add_group(group_step, far_sum):
        first_slot = group_step * group_size
        rows_group = lax.dynamic_slice_in_dim(rows_local, first_slot, group_size)
        cols_group = lax.dynamic_slice_in_dim(cols_local, first_slot, group_size)
        rank_group = lax.dynamic_slice_in_dim(rank_local, first_slot, group_size)
        v_group = lax.dynamic_slice_in_dim(v_wave, first_slot, group_size, 0)
        u_group = lax.dynamic_slice_in_dim(u_wave, first_slot, group_size, 0)
        slot_tiles = jnp.take(wave_tiles, cols_group, axis=0)
        real_prod = jnp.einsum(
            "fkq,fqc->fkc", v_group[:, 0], slot_tiles, preferred_element_type=jnp.float32
        )
        imag_prod = jnp.einsum(
            "fkq,fqc->fkc", v_group[:, 1], slot_tiles, preferred_element_type=jnp.float32
        )
        live_mask = (first_slot + slot_ids < live_count)[:, None] & (
            rank_ids[None, :] < rank_group[:, None]
        )
        coefficients = (
            combine_parts(real_prod, imag_prod) * live_mask[:, :, None].astype(jnp.float32)
        ).astype(jnp.bfloat16)
        real_back = jnp.einsum(
            "fkp,fkc->fpc", u_group[:, 0], coefficients, preferred_element_type=jnp.float32
        )
        imag_back = jnp.einsum(
            "fkp,fkc->fpc", u_group[:, 1], coefficients, preferred_element_type=jnp.float32
        )
        contrib = combine_parts(real_back, imag_back)
        return far_sum.at[rows_group].add(contrib)

    zero_sum = jnp.zeros((row_blocks, tile_rows, columns), jnp.float32)
    return lax.fori_loop(0, group_limit, add_group, zero_sum)


def reduce_rows(far_sum, row_blocks, tile_rows, columns):
    flat_rows = far_sum.reshape(row_blocks * tile_rows, columns)
    return lax.psum_scatter(flat_rows, "col", scatter_dimension=0, tiled=True)


def generic_shards(incident, near_tiles, near_offsets, far_row, far_col, far_rank, far_count, far_u, far_v):
    wave_count, tile_rows, columns = incident.shape
    row_blocks = lax.axis_size("col")
    slot_count = far_row.shape[2]
    stacked = []
    for shift_by in (2, 1, 0, -1, -2):
        if shift_by == 0:
            stacked.append(incident)
        else:
            stacked.append(from_behind(incident, ("row", "col"), shift_by))
    neighbour = jnp.stack(stacked, axis=1)
    near_inputs = jnp.take(neighbour, near_offsets[0] + 2, axis=1)
    local_near = near_tiles[0]
    real_prod = jnp.einsum(
        "wnpq,wnqc->wpc", local_near[:, :, 0], near_inputs, preferred_element_type=jnp.float32
    )
    imag_prod = jnp.einsum(
        "wnpq,wnqc->wpc", local_near[:, :, 1], near_inputs, preferred_element_type=jnp.float32
    )
    near_total = combine_parts(real_prod, imag_prod)
    rows_local = far_row[0, 0]
    cols_local = far_col[0, 0]
    rank_local = far_rank[0, 0]
    live_count = far_count[0, 0]
    group_limit = slot_count // 16
    gathered = lax.all_gather(incident, "row", axis=1, tiled=True)
    outputs = []
    for wave_index in range(wave_count):
        wave_columns = gathered[wave_index]
        wave_tiles = wave_columns.reshape(-1, tile_rows, columns)
        far_sum = far_partial(
            wave_tiles,
            rows_local,
            cols_local,
            rank_local,
            live_count,
            far_u[0, 0, wave_index],
            far_v[0, 0, wave_index],
            group_limit,
            row_blocks,
        )
        own_rows = reduce_rows(far_sum, row_blocks, tile_rows, columns)
        outputs.append(near_total[wave_index] + own_rows)
    return jnp.stack(outputs, axis=0).astype(jnp.bfloat16)


def fused_kernel(
    depth, offset_ref, row_ref, col_ref, rank_ref, count_ref, x_hbm, near_hbm, u_hbm, v_hbm, out_hbm,
    tiles, close, near_buf, u_buf, v_buf, u_turn, u_give, coef, give, v_out, v_in, served, total, out_buf, keys, table,
    recv_sem, send_sem, pair_sem, v_send, v_recv, s_send, s_recv, g_send, g_recv, t_send, t_recv, load_sem, out_sem,
):
    waves = tiles.shape[0]
    row_count = depth * 4
    places = depth * 2
    half = depth // 2
    row_blocks = table.shape[1]
    slots = v_buf.shape[1]
    rank_rows = v_buf.shape[3]
    tile_rows = tiles.shape[2]
    r = lax.axis_index("row")
    c = lax.axis_index("col")
    z, y, x = r // 4, (r // 2) % 2, r % 2
    own_slot, edge_slot = row_count, row_count + 1
    edge_tile = (r + 1 - 2 * c + row_count) % row_count
    partner = r + 2 * (1 - 2 * y)
    has_up, has_down = z < depth - 1, z > 0
    beside = r + 1 - 2 * x
    low_end, high_end = 2, row_count - 3
    doubled = c == 1
    is_end = ((r == low_end) | (r == high_end)) & ~doubled
    is_feeder = ((beside == low_end) | (beside == high_end)) & ~doubled
    across = partner + 1 - 2 * x

    def corner_of(row):
        return (row + 2 * (row % 2) - 1 + row_count) % row_count

    def at_wrap(row):
        return (row == 0) | (row == row_count - 1)

    leaps = doubled & at_wrap(across)
    leapt = doubled & at_wrap(r)

    def serves_side(row):
        return (c >= SIDE_FROM) & ~at_wrap(row)

    corner, partner_corner = corner_of(r), corner_of(partner)

    def row_of(tz, ty, tx):
        return (tz * 2 + ty) * 2 + tx

    load_x = [
        pltpu.make_async_copy(x_hbm.at[wave], tiles.at[wave, r], load_sem.at[3 + wave])
        for wave in range(waves)
    ]
    load_v = pltpu.make_async_copy(v_hbm.at[0, 0], v_buf, load_sem.at[0])
    load_u = pltpu.make_async_copy(u_hbm.at[0, 0], u_buf, load_sem.at[1])
    load_near = pltpu.make_async_copy(near_hbm.at[0], near_buf, load_sem.at[2])
    for load in load_x + [load_v, load_u, load_near]:
        load.start()

    barrier = pltpu.get_barrier_semaphore()

    def greet(device):
        pl.semaphore_signal(barrier, inc=1, device_id=device, device_id_type=MESH)

    for device in ((partner, c), (partner, 1 - c), (beside, c), (beside, 1 - c), (r, 1 - c)):
        greet(device)

    @pl.when(leapt)
    def _():
        greet((across, c))

    @pl.when(has_up)
    def _():
        greet((row_of(z + 1, y, x), c))

    @pl.when(has_down)
    def _():
        greet((row_of(z - 1, y, x), c))

    for s in range(slots):
        key = row_ref[0, 0, s] * row_count + col_ref[0, 0, s]
        keys[s] = jnp.where(s < count_ref[0, 0], key, -1)

    def look_up(a, tile):
        wanted = a * row_count + tile
        slot, rank = jnp.int32(0), jnp.int32(0)
        for s in range(slots):
            hit = keys[s] == wanted
            slot = jnp.where(hit, s, slot)
            rank = jnp.where(hit, rank_ref[0, 0, s], rank)
        table[0, a, tile] = slot
        table[1, a, tile] = rank

    pl.semaphore_wait(barrier, 5 + jnp.where(has_up, 1, 0) + jnp.where(has_down, 1, 0) + jnp.where(leaps, 1, 0))

    def copy_to(source, target, sent, received, device):
        return pltpu.make_async_remote_copy(
            src_ref=source,
            dst_ref=target,
            send_sem=sent,
            recv_sem=received,
            device_id=device,
            device_id_type=MESH,
        )

    def hop(wave, tile, link, row):
        here = tiles.at[wave, tile]
        return copy_to(here, here, send_sem.at[link], recv_sem.at[wave, tile], (row, c))

    def along_z(wave, tile, step):
        return hop(wave, tile, (1 - step) // 2, row_of(z + step, y, x))

    def along_x(wave, tile):
        return hop(wave, tile, ALONG_X, beside)

    def along_y(wave, tile):
        return hop(wave, tile, ALONG_Y, partner)

    def leap(wave):
        return hop(wave, corner_of(across), ALONG_Y, across)

    def to_pair(wave, tile, slot):
        return copy_to(
            tiles.at[wave, tile],
            close.at[wave, slot - row_count + 2],
            pair_sem.at[0],
            recv_sem.at[wave, slot],
            (r, 1 - c),
        )

    def send_v(place):
        return copy_to(
            v_out.at[place], v_in.at[place], v_send.at[0], v_recv.at[place], (partner, c)
        )

    def send_v_side(place):
        return copy_to(
            v_out.at[place], v_in.at[places], v_send.at[0], v_recv.at[places], (beside, c)
        )

    def send_served(place, wave, j):
        return copy_to(
            served.at[place, wave, j],
            coef.at[half + place // 4, wave, j, place % 4],
            s_send.at[0],
            s_recv.at[place // 4],
            (partner, c if j == 0 else 1 - c),
        )

    def send_served_side(place, wave, j):
        return copy_to(
            served.at[places, wave, j],
            coef.at[half + place // 4, wave, j, place % 4],
            s_send.at[0],
            s_recv.at[place // 4],
            (beside, c if j == 0 else 1 - c),
        )

    def send_give(plane, place, index):
        return copy_to(
            give.at[index],
            coef.at[plane * half + place // 4, :, 1, place % 4],
            g_send.at[0],
            g_recv.at[half if plane else place // 4],
            (r, 1 - c),
        )

    def send_turn(chunk):
        return copy_to(
            u_give.at[chunk],
            u_turn.at[chunk, :, :, pl.ds(4 * rank_rows, 4 * rank_rows)],
            t_send.at[0],
            t_recv.at[chunk],
            (r, 1 - c),
        )

    middle = jnp.minimum(z, depth - 1 - z)

    def level_of(step):
        reach = (step + 1) // 2
        near_level = z + jnp.where(step % 2 == 1, reach, -reach)
        beyond = step - middle
        far_level = z + jnp.where(depth - 1 - z > z, beyond, -beyond)
        return jnp.where(step <= 2 * middle, near_level, far_level)

    def tile_at(plane, place):
        level, other = level_of(place // 2), place % 2
        return row_of(level, y + plane - 2 * y * plane, x + other - 2 * x * other)

    def complex_rows(prod, at):
        at = 2 * rank_rows * at
        return combine_parts(prod[at:at + rank_rows], prod[at + rank_rows:at + 2 * rank_rows])

    def project(plane, place, tile, index, wave):
        factors = [v_buf[wave, table[0, a, tile]].reshape(2 * rank_rows, -1) for a in (c, 1 - c)]
        prod = jnp.dot(
            jnp.concatenate(factors, axis=0), tiles[wave, tile], preferred_element_type=jnp.float32
        )
        chunk = plane * half + place // 4
        coef[chunk, wave, 0, place % 4] = complex_rows(prod, 0).astype(jnp.bfloat16)
        give[index, wave] = complex_rows(prod, 1).astype(jnp.bfloat16)
        if wave == waves - 1:
            send_give(plane, place, index).start()

    def serve(place, tile, wave, send):
        left = v_in[place, wave].reshape(row_blocks * 2 * rank_rows, -1)
        prod = jnp.dot(left, tiles[wave, tile], preferred_element_type=jnp.float32)
        for j in range(row_blocks):
            served[place, wave, j] = complex_rows(prod, j).astype(jnp.bfloat16)
        for j in range(row_blocks):
            send(wave, j).start()

    def await_bytes(part, sem):
        pltpu.make_async_copy(part, part, sem).wait()

    def arrive(wave, tile):
        await_bytes(tiles.at[wave, r], recv_sem.at[wave, tile])

    def share_edge(wave, tile):
        @pl.when(tile == edge_tile)
        def _():
            to_pair(wave, tile, edge_slot).start()

    for wave in range(waves):
        load_x[wave].wait()
        along_x(wave, r).start()

        @pl.when(has_up)
        def _():
            along_z(wave, r, 1).start()

        @pl.when(has_down)
        def _():
            along_z(wave, r, -1).start()

        to_pair(wave, r, own_slot).start()

    load_v.wait()

    def push_v(place, carry):
        tile = tile_at(1, place)
        for a in range(row_blocks):
            look_up(a, tile)

        @pl.when(tile != corner)
        def _():
            for wave in range(waves):
                for j, a in enumerate((c, 1 - c)):
                    v_out[place, wave, j] = v_buf[wave, table[0, a, tile]]
            aside = (tile == corner_of(beside)) & serves_side(beside)

            @pl.when(aside)
            def _():
                send_v_side(place).start()

            @pl.when(~aside)
            def _():
                send_v(place).start()

        return carry

    lax.fori_loop(0, places, push_v, 0)

    def find_own(place, carry):
        for a in range(row_blocks):
            look_up(a, tile_at(0, place))
        return carry

    lax.fori_loop(0, places, find_own, 0)
    load_u.wait()
    load_near.wait()
    rank_ids = lax.broadcasted_iota(jnp.int32, (rank_rows, tile_rows), 0)

    def place_u(chunk):
        plane, first = chunk // half, (chunk % half) * 4
        for wave in range(waves):
            for j, a in enumerate((c, 1 - c)):
                for part in range(2):
                    rows = []
                    for at in range(4):
                        tile = tile_at(plane, first + at)
                        factor = u_buf[wave, table[0, a, tile], part].astype(jnp.float32)
                        rows.append(jnp.where(rank_ids < table[1, a, tile], factor, 0.0))
                    flipped = jnp.concatenate(rows, axis=0).T.astype(jnp.bfloat16)
                    lines = pl.ds(part * tile_rows, tile_rows)
                    if j == 0:
                        u_turn[chunk, wave, lines, 0:4 * rank_rows] = flipped
                    else:
                        u_give[chunk, wave, lines, :] = flipped
        send_turn(chunk).start()

    def served_here(tile):
        return (tile != partner_corner) & ~((tile == corner_of(across)) & serves_side(across))

    def use_tile(place, tile, wave):
        @pl.when(served_here(tile))
        def _():
            if wave == 0:
                send_v(place).wait_recv()
            serve(place, tile, wave, functools.partial(send_served, place))

        project(0, place, tile, place, wave)

    def at_end(level):
        return (level == 0) | (level == depth - 1)

    def forward(step, tile, wave):
        level = level_of(step)
        arrive(wave, tile)

        @pl.when(leaps & (tile == corner_of(across)))
        def _():
            leap(wave).start()

        @pl.when((level < z) & has_up)
        def _():
            along_z(wave, tile, 1).start()

        @pl.when((level > z) & has_down)
        def _():
            along_z(wave, tile, -1).start()

        held = wave == waves - 1

        crosses = ~(is_feeder & (step == depth - 2)) if held else step > 0

        @pl.when(crosses & ~(doubled & at_end(level)))
        def _():
            along_x(wave, tile).start()

        if held:
            @pl.when(is_feeder & (step == depth - 1))
            def _():
                along_x(wave, tile_at(0, 2 * step - 2)).start()

    def take_side(place, wave):
        tile = tile_at(0, place)
        arrive(wave, tile)
        share_edge(wave, tile)
        level = level_of(place // 2)
        passes = doubled & at_end(level)

        @pl.when(passes & (level <= z) & has_up)
        def _():
            along_z(wave, tile, 1).start()

        @pl.when(passes & (level >= z) & has_down)
        def _():
            along_z(wave, tile, -1).start()

        @pl.when((tile == partner_corner) & ~(doubled & at_wrap(partner)))
        def _():
            along_y(wave, tile).start()

    corner_place = 1
    for step in range(depth):
        corner_place += jnp.where(row_of(level_of(step), 1 - y, 1 - x) == corner, 2 * step, 0)

    def use_corner():
        for wave in range(waves):
            arrive(wave, corner)
            share_edge(wave, corner)

            @pl.when(serves_side(r))
            def _():
                if wave == 0:
                    send_v_side(0).wait_recv()
                serve(places, corner, wave, functools.partial(send_served_side, corner_place - 1))

            project(1, corner_place, corner, places, wave)

    def far_chunk(chunk, wave):
        right = coef[chunk, wave].reshape(-1, coef.shape[-1])
        return jnp.dot(u_turn[chunk, wave], right, preferred_element_type=jnp.float32)

    def place_of(offset):
        across_chip = jnp.where(offset == 1 - 2 * c, 2, 3)
        return jnp.where(offset % 2 == 0, jnp.where(offset == 2 * (beside - r), 0, 1), across_chip)

    def near_sum(wave):
        value = None
        for n in range(near_buf.shape[1]):
            left = near_buf[wave, n].reshape(2 * tile_rows, tile_rows)
            block = close[wave, place_of(offset_ref[0, n])] if n else tiles[wave, r]
            prod = jnp.dot(left, block, preferred_element_type=jnp.float32)
            value = prod if value is None else value + prod
        return value

    def await_chunk(chunk):
        await_bytes(u_give.at[0], t_recv.at[chunk])
        part = coef.at[chunk]
        if chunk < half:
            await_bytes(part.at[:, 1], g_recv.at[chunk])
        else:
            sem = s_recv.at[chunk - half]
            holds_corner = corner_place // 4 == chunk - half

            @pl.when(holds_corner)
            def _():
                await_bytes(part.at[:, :, 0:3], sem)
                await_bytes(give.at[0], g_recv.at[half])

            @pl.when(~holds_corner)
            def _():
                await_bytes(part, sem)

    def add_chunk(chunk):
        await_chunk(chunk)
        for wave in range(waves):
            total[wave] += far_chunk(chunk, wave)

    def await_near():
        for wave in range(waves):
            arrive(wave, own_slot)
            arrive(wave, edge_slot)
            close[wave, 0] = tiles[wave, beside]
            close[wave, 1] = tiles[wave, corner]

    def await_first():
        for chunk in range(half - 1):
            await_chunk(chunk)

    def first_sum(with_near, wave, carry):
        value = near_sum(wave) if with_near else jnp.zeros(total.shape[1:], jnp.float32)
        for chunk in range(half - 1):
            value += far_chunk(chunk, wave)
        total[wave] = value
        return carry

    def add_near(wave, carry):
        total[wave] += near_sum(wave)
        return carry

    def put_out(wave):
        return pltpu.make_async_copy(out_buf.at[wave], out_hbm.at[wave], out_sem.at[wave])

    def comes_early(step):
        return doubled & has_up & has_down & at_end(level_of(step))

    def spread(distance, carry):
        behind = 2 * distance - 1

        @pl.when(distance < depth)
        def _():
            place_u(distance)

        @pl.when(distance == 0)
        def _():
            for wave in range(waves):
                use_tile(0, r, wave)

        @pl.when((distance == depth) & ~at_wrap(r))
        def _():
            use_corner()
            await_near()
            await_first()
            lax.fori_loop(0, waves, functools.partial(first_sum, True), 0)

        @pl.when(distance > 0)
        def _():
            for wave in range(waves):
                for sign in (1, -1):
                    level = z + sign * distance

                    @pl.when((level >= 0) & (level < depth))
                    def _():
                        first = 2 * distance - (1 if sign == 1 else 0)
                        step = jnp.where(distance <= middle, first, middle + distance)
                        tile = row_of(level, y, x)
                        forward(step, tile, wave)
                        use_tile(2 * step, tile, wave)

                if wave == waves - 1:
                    @pl.when(is_end & (distance == depth - 1))
                    def _():
                        for early in range(waves):
                            take_side(places - 1, early)

                @pl.when(~comes_early(distance - 1))
                def _():
                    @pl.when(~(is_end & (distance == depth)))
                    def _():
                        take_side(behind, wave)

                    use_tile(behind, tile_at(0, behind), wave)

                @pl.when(comes_early(distance) & (distance < depth))
                def _():
                    take_side(behind + 2, wave)
                    use_tile(behind + 2, tile_at(0, behind + 2), wave)

        return carry

    lax.fori_loop(0, depth + 1, spread, 0)

    @pl.when(at_wrap(r))
    def _():
        await_first()
        lax.fori_loop(0, waves, functools.partial(first_sum, False), 0)

    add_chunk(half - 1)
    for chunk in range(half, depth - 1):
        add_chunk(chunk)

    @pl.when(at_wrap(r))
    def _():
        use_corner()
        await_near()
        lax.fori_loop(0, waves, add_near, 0)

    await_chunk(depth - 1)
    for wave in range(waves):
        value = total[wave] + far_chunk(depth - 1, wave)
        out_buf[wave] = combine_parts(value[:tile_rows], value[tile_rows:]).astype(out_buf.dtype)
        put_out(wave).start()

    def await_count(parts, count, most, sem):
        for n in range(1, most + 1):
            @pl.when(count == n)
            def _():
                await_bytes(parts(n), sem)

    def one_if(flag):
        return jnp.where(flag, 1, 0)

    def some_tiles(n):
        return tiles.at[:, 0:n]

    def ends_but(level):
        return one_if(doubled) * (2 - one_if(at_end(level)))

    await_bytes(some_tiles(2), pair_sem.at[0])
    await_bytes(v_out.at[0:places - 1], v_send.at[0])
    await_bytes(give, g_send.at[0])
    await_bytes(u_give, t_send.at[0])
    sides = places - 1 - one_if(serves_side(across)) + one_if(serves_side(r))
    await_count(lambda n: served.at[0:n], sides, places, s_send.at[0])
    ups = one_if(has_up) * (z + 1 + one_if(doubled))
    await_count(some_tiles, ups, depth, send_sem.at[UP])
    downs = one_if(has_down) * (depth - z + one_if(doubled))
    await_count(some_tiles, downs, depth, send_sem.at[DOWN])
    await_count(some_tiles, depth - ends_but(z), depth, send_sem.at[ALONG_X])
    lines = one_if(leaps) + one_if(~(doubled & at_wrap(partner)))
    await_count(some_tiles, lines, 2, send_sem.at[ALONG_Y])
    for wave in range(waves):
        put_out(wave).wait()


def fused_shards(incident, near_tiles, near_offsets, far_row, far_col, far_rank, far_count, far_u, far_v):
    waves, tile_rows, columns = incident.shape
    row_count, row_blocks = lax.axis_size("row"), lax.axis_size("col")
    slots, rank_rows = far_u.shape[3], far_u.shape[5]
    near_slots = near_tiles.shape[2]
    depth, places, half = row_count // 4, row_count // 2, row_count // 8
    bf16, f32 = jnp.bfloat16, jnp.float32
    any_space = pl.BlockSpec(memory_space=pl.ANY)
    smem = pl.BlockSpec(memory_space=pltpu.SMEM)
    dma = pltpu.SemaphoreType.DMA
    return pl.pallas_call(
        functools.partial(fused_kernel, depth),
        out_shape=jax.ShapeDtypeStruct(incident.shape, bf16),
        in_specs=[smem] * 5 + [any_space] * 4,
        out_specs=any_space,
        scratch_shapes=[
            pltpu.VMEM((waves, row_count, tile_rows, columns), bf16),
            pltpu.VMEM((waves, 4, tile_rows, columns), bf16),
            pltpu.VMEM((waves, near_slots, 2, tile_rows, tile_rows), bf16),
            pltpu.VMEM((waves, slots, 2, rank_rows, tile_rows), bf16),
            pltpu.VMEM((waves, slots, 2, rank_rows, tile_rows), bf16),
            pltpu.VMEM((depth, waves, 2 * tile_rows, 8 * rank_rows), bf16),
            pltpu.VMEM((depth, waves, 2 * tile_rows, 4 * rank_rows), bf16),
            pltpu.VMEM((depth, waves, row_blocks, 4, rank_rows, columns), bf16),
            pltpu.VMEM((places + 1, waves, rank_rows, columns), bf16),
            pltpu.VMEM((places, waves, row_blocks, 2, rank_rows, tile_rows), bf16),
            pltpu.VMEM((places + 1, waves, row_blocks, 2, rank_rows, tile_rows), bf16),
            pltpu.VMEM((places + 1, waves, row_blocks, rank_rows, columns), bf16),
            pltpu.VMEM((waves, 2 * tile_rows, columns), f32),
            pltpu.VMEM(incident.shape, bf16),
            pltpu.SMEM((slots,), jnp.int32),
            pltpu.SMEM((2, row_blocks, row_count), jnp.int32),
            dma((waves, row_count + 2)),
            dma((4,)),
            dma((1,)),
            dma((1,)),
            dma((places + 1,)),
            dma((1,)),
            dma((half,)),
            dma((1,)),
            dma((half + 1,)),
            dma((1,)),
            dma((depth,)),
            dma((3 + waves,)),
            dma((waves,)),
        ],
        compiler_params=pltpu.CompilerParams(collective_id=0, has_side_effects=True),
    )(near_offsets, far_row, far_col, far_rank, far_count, incident, near_tiles, far_u, far_v)


def solution(mesh):
    in_specs = (
        P(None, ("row", "col"), None),
        P(("row", "col"), None, None, None, None, None),
        P(("row", "col"), None),
        P("row", "col", None),
        P("row", "col", None),
        P("row", "col", None),
        P("row", "col"),
        P("row", "col", None, None, None, None, None),
        P("row", "col", None, None, None, None, None),
    )
    out_specs = P(None, ("row", "col"), None)
    paired = mesh.shape["col"] == 2 and mesh.shape["row"] % 8 == 0
    shards = fused_shards if paired else generic_shards
    return jax.shard_map(shards, mesh=mesh, in_specs=in_specs, out_specs=out_specs, check_vma=False)
```

```python
import functools

import jax
import jax.numpy as jnp
from jax import lax
from jax.experimental import pallas as pl
from jax.experimental.pallas import tpu as pltpu
from jax.sharding import PartitionSpec as P

MESH = pl.DeviceIdType.MESH
UP, DOWN, ALONG_Y, ALONG_X = range(4)


def from_behind(value, axis, steps):
    count = lax.axis_size(axis)
    pairs = [(source, (source + steps) % count) for source in range(count)]
    return lax.ppermute(value, axis, pairs)


def combine_parts(real_prod, imag_prod):
    half_width = real_prod.shape[-1] // 2
    return jnp.concatenate(
        [
            real_prod[..., :half_width] - imag_prod[..., half_width:],
            real_prod[..., half_width:] + imag_prod[..., :half_width],
        ],
        axis=-1,
    )


def far_partial(
    wave_tiles,
    rows_local,
    cols_local,
    rank_local,
    live_count,
    u_wave,
    v_wave,
    group_limit,
    row_blocks,
):
    group_size = 16
    tile_rows = wave_tiles.shape[1]
    columns = wave_tiles.shape[2]
    rank_size = v_wave.shape[2]
    slot_ids = jnp.arange(group_size, dtype=jnp.int32)
    rank_ids = jnp.arange(rank_size, dtype=jnp.int32)

    def add_group(group_step, far_sum):
        first_slot = group_step * group_size
        rows_group = lax.dynamic_slice_in_dim(rows_local, first_slot, group_size)
        cols_group = lax.dynamic_slice_in_dim(cols_local, first_slot, group_size)
        rank_group = lax.dynamic_slice_in_dim(rank_local, first_slot, group_size)
        v_group = lax.dynamic_slice_in_dim(v_wave, first_slot, group_size, 0)
        u_group = lax.dynamic_slice_in_dim(u_wave, first_slot, group_size, 0)
        slot_tiles = jnp.take(wave_tiles, cols_group, axis=0)
        real_prod = jnp.einsum(
            "fkq,fqc->fkc", v_group[:, 0], slot_tiles, preferred_element_type=jnp.float32
        )
        imag_prod = jnp.einsum(
            "fkq,fqc->fkc", v_group[:, 1], slot_tiles, preferred_element_type=jnp.float32
        )
        live_mask = (first_slot + slot_ids < live_count)[:, None] & (
            rank_ids[None, :] < rank_group[:, None]
        )
        coefficients = (
            combine_parts(real_prod, imag_prod) * live_mask[:, :, None].astype(jnp.float32)
        ).astype(jnp.bfloat16)
        real_back = jnp.einsum(
            "fkp,fkc->fpc", u_group[:, 0], coefficients, preferred_element_type=jnp.float32
        )
        imag_back = jnp.einsum(
            "fkp,fkc->fpc", u_group[:, 1], coefficients, preferred_element_type=jnp.float32
        )
        contrib = combine_parts(real_back, imag_back)
        return far_sum.at[rows_group].add(contrib)

    zero_sum = jnp.zeros((row_blocks, tile_rows, columns), jnp.float32)
    return lax.fori_loop(0, group_limit, add_group, zero_sum)


def reduce_rows(far_sum, row_blocks, tile_rows, columns):
    flat_rows = far_sum.reshape(row_blocks * tile_rows, columns)
    return lax.psum_scatter(flat_rows, "col", scatter_dimension=0, tiled=True)


def generic_shards(incident, near_tiles, near_offsets, far_row, far_col, far_rank, far_count, far_u, far_v):
    wave_count, tile_rows, columns = incident.shape
    row_blocks = lax.axis_size("col")
    slot_count = far_row.shape[2]
    stacked = []
    for shift_by in (2, 1, 0, -1, -2):
        if shift_by == 0:
            stacked.append(incident)
        else:
            stacked.append(from_behind(incident, ("row", "col"), shift_by))
    neighbour = jnp.stack(stacked, axis=1)
    near_inputs = jnp.take(neighbour, near_offsets[0] + 2, axis=1)
    local_near = near_tiles[0]
    real_prod = jnp.einsum(
        "wnpq,wnqc->wpc", local_near[:, :, 0], near_inputs, preferred_element_type=jnp.float32
    )
    imag_prod = jnp.einsum(
        "wnpq,wnqc->wpc", local_near[:, :, 1], near_inputs, preferred_element_type=jnp.float32
    )
    near_total = combine_parts(real_prod, imag_prod)
    rows_local = far_row[0, 0]
    cols_local = far_col[0, 0]
    rank_local = far_rank[0, 0]
    live_count = far_count[0, 0]
    group_limit = slot_count // 16
    gathered = lax.all_gather(incident, "row", axis=1, tiled=True)
    outputs = []
    for wave_index in range(wave_count):
        wave_columns = gathered[wave_index]
        wave_tiles = wave_columns.reshape(-1, tile_rows, columns)
        far_sum = far_partial(
            wave_tiles,
            rows_local,
            cols_local,
            rank_local,
            live_count,
            far_u[0, 0, wave_index],
            far_v[0, 0, wave_index],
            group_limit,
            row_blocks,
        )
        own_rows = reduce_rows(far_sum, row_blocks, tile_rows, columns)
        outputs.append(near_total[wave_index] + own_rows)
    return jnp.stack(outputs, axis=0).astype(jnp.bfloat16)


def fused_kernel(
    depth, offset_ref, row_ref, col_ref, rank_ref, count_ref, x_hbm, near_hbm, u_hbm, v_hbm, out_ref,
    tiles, close, near_buf, u_buf, v_buf, u_turn, u_give, coef, give, v_out, v_in, served, total, keys, table,
    recv_sem, send_sem, pair_sem, v_send, v_recv, s_send, s_recv, g_send, g_recv, t_send, t_recv, load_sem,
):
    waves = tiles.shape[0]
    row_count = depth * 4
    places = depth * 2
    half = depth // 2
    row_blocks = table.shape[1]
    slots = v_buf.shape[1]
    rank_rows = v_buf.shape[3]
    tile_rows = tiles.shape[2]
    r = lax.axis_index("row")
    c = lax.axis_index("col")
    z, y, x = r // 4, (r // 2) % 2, r % 2
    own_slot, edge_slot = row_count, row_count + 1
    edge_tile = (r + 1 - 2 * c + row_count) % row_count
    partner = r + 2 * (1 - 2 * y)
    has_up, has_down = z < depth - 1, z > 0
    beside = r + 1 - 2 * x
    low_end, high_end = 2, row_count - 3
    doubled = c == 1
    is_end = ((r == low_end) | (r == high_end)) & ~doubled
    is_feeder = ((beside == low_end) | (beside == high_end)) & ~doubled
    across = partner + 1 - 2 * x

    def corner_of(row):
        return (row + 2 * (row % 2) - 1 + row_count) % row_count

    def at_wrap(row):
        return (row == 0) | (row == row_count - 1)

    leaps = doubled & at_wrap(across)
    leapt = doubled & at_wrap(r)

    def serves_side(row):
        from_end = jnp.minimum(row, row_count - 1 - row)
        return (from_end == 1) | (from_end > 3)

    corner, partner_corner = corner_of(r), corner_of(partner)

    def row_of(tz, ty, tx):
        return (tz * 2 + ty) * 2 + tx

    load_x = [
        pltpu.make_async_copy(x_hbm.at[wave], tiles.at[wave, r], load_sem.at[3 + wave])
        for wave in range(waves)
    ]
    load_v = pltpu.make_async_copy(v_hbm.at[0, 0], v_buf, load_sem.at[0])
    load_u = pltpu.make_async_copy(u_hbm.at[0, 0], u_buf, load_sem.at[1])
    load_near = pltpu.make_async_copy(near_hbm.at[0], near_buf, load_sem.at[2])
    for load in load_x + [load_v, load_u, load_near]:
        load.start()

    barrier = pltpu.get_barrier_semaphore()

    def greet(device):
        pl.semaphore_signal(barrier, inc=1, device_id=device, device_id_type=MESH)

    for device in ((partner, c), (partner, 1 - c), (beside, c), (beside, 1 - c), (r, 1 - c)):
        greet(device)

    @pl.when(leapt)
    def _():
        greet((across, c))

    @pl.when(has_up)
    def _():
        greet((row_of(z + 1, y, x), c))

    @pl.when(has_down)
    def _():
        greet((row_of(z - 1, y, x), c))

    for s in range(slots):
        key = row_ref[0, 0, s] * row_count + col_ref[0, 0, s]
        keys[s] = jnp.where(s < count_ref[0, 0], key, -1)

    def look_up(a, tile):
        wanted = a * row_count + tile
        slot, rank = jnp.int32(0), jnp.int32(0)
        for s in range(slots):
            hit = keys[s] == wanted
            slot = jnp.where(hit, s, slot)
            rank = jnp.where(hit, rank_ref[0, 0, s], rank)
        table[0, a, tile] = slot
        table[1, a, tile] = rank

    pl.semaphore_wait(barrier, 5 + jnp.where(has_up, 1, 0) + jnp.where(has_down, 1, 0) + jnp.where(leaps, 1, 0))

    def copy_to(source, target, sent, received, device):
        return pltpu.make_async_remote_copy(
            src_ref=source,
            dst_ref=target,
            send_sem=sent,
            recv_sem=received,
            device_id=device,
            device_id_type=MESH,
        )

    def hop(wave, tile, link, row):
        here = tiles.at[wave, tile]
        return copy_to(here, here, send_sem.at[link], recv_sem.at[wave, tile], (row, c))

    def along_z(wave, tile, step):
        return hop(wave, tile, (1 - step) // 2, row_of(z + step, y, x))

    def along_x(wave, tile):
        return hop(wave, tile, ALONG_X, beside)

    def along_y(wave, tile):
        return hop(wave, tile, ALONG_Y, partner)

    def leap(wave):
        return hop(wave, corner_of(across), ALONG_Y, across)

    def to_pair(wave, tile, slot):
        return copy_to(
            tiles.at[wave, tile],
            close.at[wave, slot - row_count + 2],
            pair_sem.at[0],
            recv_sem.at[wave, slot],
            (r, 1 - c),
        )

    def send_v(place):
        return copy_to(
            v_out.at[place], v_in.at[place], v_send.at[0], v_recv.at[place], (partner, c)
        )

    def send_v_side(place):
        return copy_to(
            v_out.at[place], v_in.at[places], v_send.at[0], v_recv.at[places], (beside, c)
        )

    def send_served(place, wave, j):
        return copy_to(
            served.at[place, wave, j],
            coef.at[half + place // 4, wave, j, place % 4],
            s_send.at[0],
            s_recv.at[place // 4],
            (partner, c if j == 0 else 1 - c),
        )

    def send_served_side(place, wave, j):
        return copy_to(
            served.at[places, wave, j],
            coef.at[half + place // 4, wave, j, place % 4],
            s_send.at[0],
            s_recv.at[place // 4],
            (beside, c if j == 0 else 1 - c),
        )

    def send_give(plane, place, index):
        return copy_to(
            give.at[index],
            coef.at[plane * half + place // 4, :, 1, place % 4],
            g_send.at[0],
            g_recv.at[half if plane else place // 4],
            (r, 1 - c),
        )

    def send_turn(chunk):
        return copy_to(
            u_give.at[chunk],
            u_turn.at[chunk, :, :, pl.ds(4 * rank_rows, 4 * rank_rows)],
            t_send.at[0],
            t_recv.at[chunk],
            (r, 1 - c),
        )

    middle = jnp.minimum(z, depth - 1 - z)

    def level_of(step):
        reach = (step + 1) // 2
        near_level = z + jnp.where(step % 2 == 1, reach, -reach)
        beyond = step - middle
        far_level = z + jnp.where(depth - 1 - z > z, beyond, -beyond)
        return jnp.where(step <= 2 * middle, near_level, far_level)

    def tile_at(plane, place):
        level, other = level_of(place // 2), place % 2
        return row_of(level, y + plane - 2 * y * plane, x + other - 2 * x * other)

    def complex_rows(prod, at):
        at = 2 * rank_rows * at
        return combine_parts(prod[at:at + rank_rows], prod[at + rank_rows:at + 2 * rank_rows])

    def project(plane, place, tile, index, wave):
        factors = [v_buf[wave, table[0, a, tile]].reshape(2 * rank_rows, -1) for a in (c, 1 - c)]
        prod = jnp.dot(
            jnp.concatenate(factors, axis=0), tiles[wave, tile], preferred_element_type=jnp.float32
        )
        chunk = plane * half + place // 4
        coef[chunk, wave, 0, place % 4] = complex_rows(prod, 0).astype(jnp.bfloat16)
        give[index, wave] = complex_rows(prod, 1).astype(jnp.bfloat16)
        if wave == waves - 1:
            send_give(plane, place, index).start()

    def serve(place, tile, wave, send):
        left = v_in[place, wave].reshape(row_blocks * 2 * rank_rows, -1)
        prod = jnp.dot(left, tiles[wave, tile], preferred_element_type=jnp.float32)
        for j in range(row_blocks):
            served[place, wave, j] = complex_rows(prod, j).astype(jnp.bfloat16)
        for j in range(row_blocks):
            send(wave, j).start()

    def await_bytes(part, sem):
        pltpu.make_async_copy(part, part, sem).wait()

    def arrive(wave, tile):
        await_bytes(tiles.at[wave, r], recv_sem.at[wave, tile])

    def share_edge(wave, tile):
        @pl.when(tile == edge_tile)
        def _():
            to_pair(wave, tile, edge_slot).start()

    for wave in range(waves):
        load_x[wave].wait()
        along_x(wave, r).start()

        @pl.when(has_up)
        def _():
            along_z(wave, r, 1).start()

        @pl.when(has_down)
        def _():
            along_z(wave, r, -1).start()

        to_pair(wave, r, own_slot).start()

    load_v.wait()

    def push_v(place, carry):
        tile = tile_at(1, place)
        for a in range(row_blocks):
            look_up(a, tile)

        @pl.when(tile != corner)
        def _():
            for wave in range(waves):
                for j, a in enumerate((c, 1 - c)):
                    v_out[place, wave, j] = v_buf[wave, table[0, a, tile]]
            aside = (tile == corner_of(beside)) & serves_side(beside)

            @pl.when(aside)
            def _():
                send_v_side(place).start()

            @pl.when(~aside)
            def _():
                send_v(place).start()

        return carry

    lax.fori_loop(0, places, push_v, 0)

    def find_own(place, carry):
        for a in range(row_blocks):
            look_up(a, tile_at(0, place))
        return carry

    lax.fori_loop(0, places, find_own, 0)
    load_u.wait()
    load_near.wait()
    rank_ids = lax.broadcasted_iota(jnp.int32, (rank_rows, tile_rows), 0)

    def place_u(chunk):
        plane, first = chunk // half, (chunk % half) * 4
        for wave in range(waves):
            for j, a in enumerate((c, 1 - c)):
                for part in range(2):
                    rows = []
                    for at in range(4):
                        tile = tile_at(plane, first + at)
                        factor = u_buf[wave, table[0, a, tile], part].astype(jnp.float32)
                        rows.append(jnp.where(rank_ids < table[1, a, tile], factor, 0.0))
                    flipped = jnp.concatenate(rows, axis=0).T.astype(jnp.bfloat16)
                    lines = pl.ds(part * tile_rows, tile_rows)
                    if j == 0:
                        u_turn[chunk, wave, lines, 0:4 * rank_rows] = flipped
                    else:
                        u_give[chunk, wave, lines, :] = flipped
        send_turn(chunk).start()

    def served_here(tile):
        return (tile != partner_corner) & ~((tile == corner_of(across)) & serves_side(across))

    def use_tile(place, tile, wave):
        @pl.when(served_here(tile))
        def _():
            if wave == 0:
                send_v(place).wait_recv()
            serve(place, tile, wave, functools.partial(send_served, place))

        project(0, place, tile, place, wave)

    def at_end(level):
        return (level == 0) | (level == depth - 1)

    def forward(step, tile, wave):
        level = level_of(step)
        arrive(wave, tile)

        @pl.when(leaps & (tile == corner_of(across)))
        def _():
            leap(wave).start()

        @pl.when((level < z) & has_up)
        def _():
            along_z(wave, tile, 1).start()

        @pl.when((level > z) & has_down)
        def _():
            along_z(wave, tile, -1).start()

        held = wave == waves - 1

        crosses = ~(is_feeder & (step == depth - 2)) if held else step > 0

        @pl.when(crosses & ~(doubled & at_end(level)))
        def _():
            along_x(wave, tile).start()

        if held:
            @pl.when(is_feeder & (step == depth - 1))
            def _():
                along_x(wave, tile_at(0, 2 * step - 2)).start()

    def take_side(place, wave):
        tile = tile_at(0, place)
        arrive(wave, tile)
        share_edge(wave, tile)
        level = level_of(place // 2)
        passes = doubled & at_end(level)

        @pl.when(passes & (level <= z) & has_up)
        def _():
            along_z(wave, tile, 1).start()

        @pl.when(passes & (level >= z) & has_down)
        def _():
            along_z(wave, tile, -1).start()

        @pl.when((tile == partner_corner) & ~(doubled & at_wrap(partner)))
        def _():
            along_y(wave, tile).start()

    corner_place = 1
    for step in range(depth):
        corner_place += jnp.where(row_of(level_of(step), 1 - y, 1 - x) == corner, 2 * step, 0)

    def use_corner():
        for wave in range(waves):
            arrive(wave, corner)
            share_edge(wave, corner)

            @pl.when(serves_side(r))
            def _():
                if wave == 0:
                    send_v_side(0).wait_recv()
                serve(places, corner, wave, functools.partial(send_served_side, corner_place - 1))

            project(1, corner_place, corner, places, wave)

    def far_chunk(chunk, wave):
        right = coef[chunk, wave].reshape(-1, coef.shape[-1])
        return jnp.dot(u_turn[chunk, wave], right, preferred_element_type=jnp.float32)

    def place_of(offset):
        across_chip = jnp.where(offset == 1 - 2 * c, 2, 3)
        return jnp.where(offset % 2 == 0, jnp.where(offset == 2 * (beside - r), 0, 1), across_chip)

    def near_sum(wave):
        value = None
        for n in range(near_buf.shape[1]):
            left = near_buf[wave, n].reshape(2 * tile_rows, tile_rows)
            block = close[wave, place_of(offset_ref[0, n])] if n else tiles[wave, r]
            prod = jnp.dot(left, block, preferred_element_type=jnp.float32)
            value = prod if value is None else value + prod
        return value

    def await_chunk(chunk):
        await_bytes(u_give.at[0], t_recv.at[chunk])
        part = coef.at[chunk]
        if chunk < half:
            await_bytes(part.at[:, 1], g_recv.at[chunk])
        else:
            sem = s_recv.at[chunk - half]
            holds_corner = corner_place // 4 == chunk - half

            @pl.when(holds_corner)
            def _():
                await_bytes(part.at[:, :, 0:3], sem)
                await_bytes(give.at[0], g_recv.at[half])

            @pl.when(~holds_corner)
            def _():
                await_bytes(part, sem)

    def add_chunk(chunk):
        await_chunk(chunk)
        for wave in range(waves):
            total[wave] += far_chunk(chunk, wave)

    def await_near():
        for wave in range(waves):
            arrive(wave, own_slot)
            arrive(wave, edge_slot)
            close[wave, 0] = tiles[wave, beside]
            close[wave, 1] = tiles[wave, corner]

    def await_first():
        for chunk in range(half - 1):
            await_chunk(chunk)

    def first_sum(with_near, wave, carry):
        value = near_sum(wave) if with_near else jnp.zeros(total.shape[1:], jnp.float32)
        for chunk in range(half - 1):
            value += far_chunk(chunk, wave)
        total[wave] = value
        return carry

    def add_near(wave, carry):
        total[wave] += near_sum(wave)
        return carry

    def comes_early(step):
        return doubled & has_up & has_down & at_end(level_of(step))

    def spread(distance, carry):
        behind = 2 * distance - 1

        @pl.when(distance < depth)
        def _():
            place_u(distance)

        @pl.when(distance == 0)
        def _():
            for wave in range(waves):
                use_tile(0, r, wave)

        @pl.when((distance == depth) & ~at_wrap(r))
        def _():
            use_corner()
            await_near()
            await_first()
            lax.fori_loop(0, waves, functools.partial(first_sum, True), 0)

        @pl.when(distance > 0)
        def _():
            for wave in range(waves):
                for sign in (1, -1):
                    level = z + sign * distance

                    @pl.when((level >= 0) & (level < depth))
                    def _():
                        first = 2 * distance - (1 if sign == 1 else 0)
                        step = jnp.where(distance <= middle, first, middle + distance)
                        tile = row_of(level, y, x)
                        forward(step, tile, wave)
                        use_tile(2 * step, tile, wave)

                if wave == waves - 1:
                    @pl.when(is_end & (distance == depth - 1))
                    def _():
                        for early in range(waves):
                            take_side(places - 1, early)

                @pl.when(~comes_early(distance - 1))
                def _():
                    @pl.when(~(is_end & (distance == depth)))
                    def _():
                        take_side(behind, wave)

                    use_tile(behind, tile_at(0, behind), wave)

                @pl.when(comes_early(distance) & (distance < depth))
                def _():
                    take_side(behind + 2, wave)
                    use_tile(behind + 2, tile_at(0, behind + 2), wave)

        return carry

    lax.fori_loop(0, depth + 1, spread, 0)

    @pl.when(at_wrap(r))
    def _():
        await_first()
        lax.fori_loop(0, waves, functools.partial(first_sum, False), 0)

    add_chunk(half - 1)
    for chunk in range(half, depth - 1):
        add_chunk(chunk)

    @pl.when(at_wrap(r))
    def _():
        use_corner()
        await_near()
        lax.fori_loop(0, waves, add_near, 0)

    await_chunk(depth - 1)
    for wave in range(waves):
        value = total[wave] + far_chunk(depth - 1, wave)
        out_ref[wave] = combine_parts(value[:tile_rows], value[tile_rows:]).astype(out_ref.dtype)

    def await_count(parts, count, most, sem):
        for n in range(1, most + 1):
            @pl.when(count == n)
            def _():
                await_bytes(parts(n), sem)

    def one_if(flag):
        return jnp.where(flag, 1, 0)

    def some_tiles(n):
        return tiles.at[:, 0:n]

    def ends_but(level):
        return one_if(doubled) * (2 - one_if(at_end(level)))

    await_bytes(some_tiles(2), pair_sem.at[0])
    await_bytes(v_out.at[0:places - 1], v_send.at[0])
    await_bytes(give, g_send.at[0])
    await_bytes(u_give, t_send.at[0])
    sides = places - 1 - one_if(serves_side(across)) + one_if(serves_side(r))
    await_count(lambda n: served.at[0:n], sides, places, s_send.at[0])
    ups = one_if(has_up) * (z + 1 + one_if(doubled))
    await_count(some_tiles, ups, depth, send_sem.at[UP])
    downs = one_if(has_down) * (depth - z + one_if(doubled))
    await_count(some_tiles, downs, depth, send_sem.at[DOWN])
    await_count(some_tiles, depth - ends_but(z), depth, send_sem.at[ALONG_X])
    lines = one_if(leaps) + one_if(~(doubled & at_wrap(partner)))
    await_count(some_tiles, lines, 2, send_sem.at[ALONG_Y])


def fused_shards(incident, near_tiles, near_offsets, far_row, far_col, far_rank, far_count, far_u, far_v):
    waves, tile_rows, columns = incident.shape
    row_count, row_blocks = lax.axis_size("row"), lax.axis_size("col")
    slots, rank_rows = far_u.shape[3], far_u.shape[5]
    near_slots = near_tiles.shape[2]
    depth, places, half = row_count // 4, row_count // 2, row_count // 8
    bf16, f32 = jnp.bfloat16, jnp.float32
    any_space = pl.BlockSpec(memory_space=pl.ANY)
    smem = pl.BlockSpec(memory_space=pltpu.SMEM)
    dma = pltpu.SemaphoreType.DMA
    return pl.pallas_call(
        functools.partial(fused_kernel, depth),
        out_shape=pltpu.VMEM(incident.shape, bf16),
        in_specs=[smem] * 5 + [any_space] * 4,
        out_specs=pl.BlockSpec(memory_space=pltpu.VMEM),
        scratch_shapes=[
            pltpu.VMEM((waves, row_count, tile_rows, columns), bf16),
            pltpu.VMEM((waves, 4, tile_rows, columns), bf16),
            pltpu.VMEM((waves, near_slots, 2, tile_rows, tile_rows), bf16),
            pltpu.VMEM((waves, slots, 2, rank_rows, tile_rows), bf16),
            pltpu.VMEM((waves, slots, 2, rank_rows, tile_rows), bf16),
            pltpu.VMEM((depth, waves, 2 * tile_rows, 8 * rank_rows), bf16),
            pltpu.VMEM((depth, waves, 2 * tile_rows, 4 * rank_rows), bf16),
            pltpu.VMEM((depth, waves, row_blocks, 4, rank_rows, columns), bf16),
            pltpu.VMEM((places + 1, waves, rank_rows, columns), bf16),
            pltpu.VMEM((places, waves, row_blocks, 2, rank_rows, tile_rows), bf16),
            pltpu.VMEM((places + 1, waves, row_blocks, 2, rank_rows, tile_rows), bf16),
            pltpu.VMEM((places + 1, waves, row_blocks, rank_rows, columns), bf16),
            pltpu.VMEM((waves, 2 * tile_rows, columns), f32),
            pltpu.SMEM((slots,), jnp.int32),
            pltpu.SMEM((2, row_blocks, row_count), jnp.int32),
            dma((waves, row_count + 2)),
            dma((4,)),
            dma((1,)),
            dma((1,)),
            dma((places + 1,)),
            dma((1,)),
            dma((half,)),
            dma((1,)),
            dma((half + 1,)),
            dma((1,)),
            dma((depth,)),
            dma((3 + waves,)),
        ],
        compiler_params=pltpu.CompilerParams(collective_id=0, has_side_effects=True),
    )(near_offsets, far_row, far_col, far_rank, far_count, incident, near_tiles, far_u, far_v)


def solution(mesh):
    in_specs = (
        P(None, ("row", "col"), None),
        P(("row", "col"), None, None, None, None, None),
        P(("row", "col"), None),
        P("row", "col", None),
        P("row", "col", None),
        P("row", "col", None),
        P("row", "col"),
        P("row", "col", None, None, None, None, None),
        P("row", "col", None, None, None, None, None),
    )
    out_specs = P(None, ("row", "col"), None)
    paired = mesh.shape["col"] == 2 and mesh.shape["row"] % 8 == 0
    shards = fused_shards if paired else generic_shards
    return jax.shard_map(shards, mesh=mesh, in_specs=in_specs, out_specs=out_specs, check_vma=False)
```

```python
import functools

import jax
import jax.numpy as jnp
from jax import lax
from jax.experimental import pallas as pl
from jax.experimental.pallas import tpu as pltpu
from jax.sharding import PartitionSpec as P

MESH = pl.DeviceIdType.MESH
UP, DOWN, ALONG_Y, ALONG_X = range(4)


def from_behind(value, axis, steps):
    count = lax.axis_size(axis)
    pairs = [(source, (source + steps) % count) for source in range(count)]
    return lax.ppermute(value, axis, pairs)


def combine_parts(real_prod, imag_prod):
    half_width = real_prod.shape[-1] // 2
    return jnp.concatenate(
        [
            real_prod[..., :half_width] - imag_prod[..., half_width:],
            real_prod[..., half_width:] + imag_prod[..., :half_width],
        ],
        axis=-1,
    )


def far_partial(
    wave_tiles,
    rows_local,
    cols_local,
    rank_local,
    live_count,
    u_wave,
    v_wave,
    group_limit,
    row_blocks,
):
    group_size = 16
    tile_rows = wave_tiles.shape[1]
    columns = wave_tiles.shape[2]
    rank_size = v_wave.shape[2]
    slot_ids = jnp.arange(group_size, dtype=jnp.int32)
    rank_ids = jnp.arange(rank_size, dtype=jnp.int32)

    def add_group(group_step, far_sum):
        first_slot = group_step * group_size
        rows_group = lax.dynamic_slice_in_dim(rows_local, first_slot, group_size)
        cols_group = lax.dynamic_slice_in_dim(cols_local, first_slot, group_size)
        rank_group = lax.dynamic_slice_in_dim(rank_local, first_slot, group_size)
        v_group = lax.dynamic_slice_in_dim(v_wave, first_slot, group_size, 0)
        u_group = lax.dynamic_slice_in_dim(u_wave, first_slot, group_size, 0)
        slot_tiles = jnp.take(wave_tiles, cols_group, axis=0)
        real_prod = jnp.einsum(
            "fkq,fqc->fkc", v_group[:, 0], slot_tiles, preferred_element_type=jnp.float32
        )
        imag_prod = jnp.einsum(
            "fkq,fqc->fkc", v_group[:, 1], slot_tiles, preferred_element_type=jnp.float32
        )
        live_mask = (first_slot + slot_ids < live_count)[:, None] & (
            rank_ids[None, :] < rank_group[:, None]
        )
        coefficients = (
            combine_parts(real_prod, imag_prod) * live_mask[:, :, None].astype(jnp.float32)
        ).astype(jnp.bfloat16)
        real_back = jnp.einsum(
            "fkp,fkc->fpc", u_group[:, 0], coefficients, preferred_element_type=jnp.float32
        )
        imag_back = jnp.einsum(
            "fkp,fkc->fpc", u_group[:, 1], coefficients, preferred_element_type=jnp.float32
        )
        contrib = combine_parts(real_back, imag_back)
        return far_sum.at[rows_group].add(contrib)

    zero_sum = jnp.zeros((row_blocks, tile_rows, columns), jnp.float32)
    return lax.fori_loop(0, group_limit, add_group, zero_sum)


def reduce_rows(far_sum, row_blocks, tile_rows, columns):
    flat_rows = far_sum.reshape(row_blocks * tile_rows, columns)
    return lax.psum_scatter(flat_rows, "col", scatter_dimension=0, tiled=True)


def generic_shards(incident, near_tiles, near_offsets, far_row, far_col, far_rank, far_count, far_u, far_v):
    wave_count, tile_rows, columns = incident.shape
    row_blocks = lax.axis_size("col")
    slot_count = far_row.shape[2]
    stacked = []
    for shift_by in (2, 1, 0, -1, -2):
        if shift_by == 0:
            stacked.append(incident)
        else:
            stacked.append(from_behind(incident, ("row", "col"), shift_by))
    neighbour = jnp.stack(stacked, axis=1)
    near_inputs = jnp.take(neighbour, near_offsets[0] + 2, axis=1)
    local_near = near_tiles[0]
    real_prod = jnp.einsum(
        "wnpq,wnqc->wpc", local_near[:, :, 0], near_inputs, preferred_element_type=jnp.float32
    )
    imag_prod = jnp.einsum(
        "wnpq,wnqc->wpc", local_near[:, :, 1], near_inputs, preferred_element_type=jnp.float32
    )
    near_total = combine_parts(real_prod, imag_prod)
    rows_local = far_row[0, 0]
    cols_local = far_col[0, 0]
    rank_local = far_rank[0, 0]
    live_count = far_count[0, 0]
    group_limit = slot_count // 16
    gathered = lax.all_gather(incident, "row", axis=1, tiled=True)
    outputs = []
    for wave_index in range(wave_count):
        wave_columns = gathered[wave_index]
        wave_tiles = wave_columns.reshape(-1, tile_rows, columns)
        far_sum = far_partial(
            wave_tiles,
            rows_local,
            cols_local,
            rank_local,
            live_count,
            far_u[0, 0, wave_index],
            far_v[0, 0, wave_index],
            group_limit,
            row_blocks,
        )
        own_rows = reduce_rows(far_sum, row_blocks, tile_rows, columns)
        outputs.append(near_total[wave_index] + own_rows)
    return jnp.stack(outputs, axis=0).astype(jnp.bfloat16)


def fused_kernel(
    depth, offset_hbm, row_hbm, col_hbm, rank_hbm, count_hbm, x_hbm, near_hbm, u_hbm, v_hbm, out_ref,
    tiles, close, near_buf, u_buf, v_buf, u_turn, u_give, coef, give, v_out, v_in, served, total, offset_ref, row_ref, col_ref, rank_ref, count_ref, keys, table,
    recv_sem, send_sem, pair_sem, v_send, v_recv, s_send, s_recv, g_send, g_recv, t_send, t_recv, load_sem,
):
    waves = tiles.shape[0]
    row_count = depth * 4
    places = depth * 2
    half = depth // 2
    row_blocks = table.shape[1]
    slots = v_buf.shape[1]
    rank_rows = v_buf.shape[3]
    tile_rows = tiles.shape[2]
    r = lax.axis_index("row")
    c = lax.axis_index("col")
    z, y, x = r // 4, (r // 2) % 2, r % 2
    own_slot, edge_slot = row_count, row_count + 1
    edge_tile = (r + 1 - 2 * c + row_count) % row_count
    partner = r + 2 * (1 - 2 * y)
    has_up, has_down = z < depth - 1, z > 0
    beside = r + 1 - 2 * x
    low_end, high_end = 2, row_count - 3
    doubled = c == 1
    is_end = ((r == low_end) | (r == high_end)) & ~doubled
    is_feeder = ((beside == low_end) | (beside == high_end)) & ~doubled
    across = partner + 1 - 2 * x

    def corner_of(row):
        return (row + 2 * (row % 2) - 1 + row_count) % row_count

    def at_wrap(row):
        return (row == 0) | (row == row_count - 1)

    leaps = doubled & at_wrap(across)
    leapt = doubled & at_wrap(r)

    def serves_side(row):
        from_end = jnp.minimum(row, row_count - 1 - row)
        return (from_end == 1) | (from_end > 3)

    corner, partner_corner = corner_of(r), corner_of(partner)

    def row_of(tz, ty, tx):
        return (tz * 2 + ty) * 2 + tx

    load_x = [
        pltpu.make_async_copy(x_hbm.at[wave], tiles.at[wave, r], load_sem.at[3 + wave])
        for wave in range(waves)
    ]
    load_v = pltpu.make_async_copy(v_hbm.at[0, 0], v_buf, load_sem.at[0])
    load_u = pltpu.make_async_copy(u_hbm.at[0, 0], u_buf, load_sem.at[1])
    load_near = pltpu.make_async_copy(near_hbm.at[0], near_buf, load_sem.at[2])
    small = (
        (row_hbm, row_ref), (col_hbm, col_ref), (rank_hbm, rank_ref),
        (count_hbm, count_ref), (offset_hbm, offset_ref),
    )
    load_small = [
        pltpu.make_async_copy(source, target, load_sem.at[3 + waves + n])
        for n, (source, target) in enumerate(small)
    ]
    for load in load_small + load_x + [load_v, load_u, load_near]:
        load.start()

    barrier = pltpu.get_barrier_semaphore()

    def greet(device):
        pl.semaphore_signal(barrier, inc=1, device_id=device, device_id_type=MESH)

    for device in ((partner, c), (partner, 1 - c), (beside, c), (beside, 1 - c), (r, 1 - c)):
        greet(device)

    @pl.when(leapt)
    def _():
        greet((across, c))

    @pl.when(has_up)
    def _():
        greet((row_of(z + 1, y, x), c))

    @pl.when(has_down)
    def _():
        greet((row_of(z - 1, y, x), c))

    for load in load_small:
        load.wait()
    for s in range(slots):
        key = row_ref[0, 0, s] * row_count + col_ref[0, 0, s]
        keys[s] = jnp.where(s < count_ref[0, 0], key, -1)

    def look_up(a, tile):
        wanted = a * row_count + tile
        slot, rank = jnp.int32(0), jnp.int32(0)
        for s in range(slots):
            hit = keys[s] == wanted
            slot = jnp.where(hit, s, slot)
            rank = jnp.where(hit, rank_ref[0, 0, s], rank)
        table[0, a, tile] = slot
        table[1, a, tile] = rank

    pl.semaphore_wait(barrier, 5 + jnp.where(has_up, 1, 0) + jnp.where(has_down, 1, 0) + jnp.where(leaps, 1, 0))

    def copy_to(source, target, sent, received, device):
        return pltpu.make_async_remote_copy(
            src_ref=source,
            dst_ref=target,
            send_sem=sent,
            recv_sem=received,
            device_id=device,
            device_id_type=MESH,
        )

    def hop(wave, tile, link, row):
        here = tiles.at[wave, tile]
        return copy_to(here, here, send_sem.at[link], recv_sem.at[wave, tile], (row, c))

    def along_z(wave, tile, step):
        return hop(wave, tile, (1 - step) // 2, row_of(z + step, y, x))

    def along_x(wave, tile):
        return hop(wave, tile, ALONG_X, beside)

    def along_y(wave, tile):
        return hop(wave, tile, ALONG_Y, partner)

    def leap(wave):
        return hop(wave, corner_of(across), ALONG_Y, across)

    def to_pair(wave, tile, slot):
        return copy_to(
            tiles.at[wave, tile],
            close.at[wave, slot - row_count + 2],
            pair_sem.at[0],
            recv_sem.at[wave, slot],
            (r, 1 - c),
        )

    def send_v(place):
        return copy_to(
            v_out.at[place], v_in.at[place], v_send.at[0], v_recv.at[place], (partner, c)
        )

    def send_v_side(place):
        return copy_to(
            v_out.at[place], v_in.at[places], v_send.at[0], v_recv.at[places], (beside, c)
        )

    def send_served(place, wave, j):
        return copy_to(
            served.at[place, wave, j],
            coef.at[half + place // 4, wave, j, place % 4],
            s_send.at[0],
            s_recv.at[place // 4],
            (partner, c if j == 0 else 1 - c),
        )

    def send_served_side(place, wave, j):
        return copy_to(
            served.at[places, wave, j],
            coef.at[half + place // 4, wave, j, place % 4],
            s_send.at[0],
            s_recv.at[place // 4],
            (beside, c if j == 0 else 1 - c),
        )

    def send_give(plane, place, index):
        return copy_to(
            give.at[index],
            coef.at[plane * half + place // 4, :, 1, place % 4],
            g_send.at[0],
            g_recv.at[half if plane else place // 4],
            (r, 1 - c),
        )

    def send_turn(chunk):
        return copy_to(
            u_give.at[chunk],
            u_turn.at[chunk, :, :, pl.ds(4 * rank_rows, 4 * rank_rows)],
            t_send.at[0],
            t_recv.at[chunk],
            (r, 1 - c),
        )

    middle = jnp.minimum(z, depth - 1 - z)

    def level_of(step):
        reach = (step + 1) // 2
        near_level = z + jnp.where(step % 2 == 1, reach, -reach)
        beyond = step - middle
        far_level = z + jnp.where(depth - 1 - z > z, beyond, -beyond)
        return jnp.where(step <= 2 * middle, near_level, far_level)

    def tile_at(plane, place):
        level, other = level_of(place // 2), place % 2
        return row_of(level, y + plane - 2 * y * plane, x + other - 2 * x * other)

    def complex_rows(prod, at):
        at = 2 * rank_rows * at
        return combine_parts(prod[at:at + rank_rows], prod[at + rank_rows:at + 2 * rank_rows])

    def project(plane, place, tile, index, wave):
        factors = [v_buf[wave, table[0, a, tile]].reshape(2 * rank_rows, -1) for a in (c, 1 - c)]
        prod = jnp.dot(
            jnp.concatenate(factors, axis=0), tiles[wave, tile], preferred_element_type=jnp.float32
        )
        chunk = plane * half + place // 4
        coef[chunk, wave, 0, place % 4] = complex_rows(prod, 0).astype(jnp.bfloat16)
        give[index, wave] = complex_rows(prod, 1).astype(jnp.bfloat16)
        if wave == waves - 1:
            send_give(plane, place, index).start()

    def serve(place, tile, wave, send):
        left = v_in[place, wave].reshape(row_blocks * 2 * rank_rows, -1)
        prod = jnp.dot(left, tiles[wave, tile], preferred_element_type=jnp.float32)
        for j in range(row_blocks):
            served[place, wave, j] = complex_rows(prod, j).astype(jnp.bfloat16)
        for j in range(row_blocks):
            send(wave, j).start()

    def await_bytes(part, sem):
        pltpu.make_async_copy(part, part, sem).wait()

    def arrive(wave, tile):
        await_bytes(tiles.at[wave, r], recv_sem.at[wave, tile])

    def share_edge(wave, tile):
        @pl.when(tile == edge_tile)
        def _():
            to_pair(wave, tile, edge_slot).start()

    for wave in range(waves):
        load_x[wave].wait()
        along_x(wave, r).start()

        @pl.when(has_up)
        def _():
            along_z(wave, r, 1).start()

        @pl.when(has_down)
        def _():
            along_z(wave, r, -1).start()

        to_pair(wave, r, own_slot).start()

    load_v.wait()

    def push_v(place, carry):
        tile = tile_at(1, place)
        for a in range(row_blocks):
            look_up(a, tile)

        @pl.when(tile != corner)
        def _():
            for wave in range(waves):
                for j, a in enumerate((c, 1 - c)):
                    v_out[place, wave, j] = v_buf[wave, table[0, a, tile]]
            aside = (tile == corner_of(beside)) & serves_side(beside)

            @pl.when(aside)
            def _():
                send_v_side(place).start()

            @pl.when(~aside)
            def _():
                send_v(place).start()

        return carry

    lax.fori_loop(0, places, push_v, 0)

    def find_own(place, carry):
        for a in range(row_blocks):
            look_up(a, tile_at(0, place))
        return carry

    lax.fori_loop(0, places, find_own, 0)
    load_u.wait()
    load_near.wait()
    rank_ids = lax.broadcasted_iota(jnp.int32, (rank_rows, tile_rows), 0)

    def place_u(chunk):
        plane, first = chunk // half, (chunk % half) * 4
        for wave in range(waves):
            for j, a in enumerate((c, 1 - c)):
                for part in range(2):
                    rows = []
                    for at in range(4):
                        tile = tile_at(plane, first + at)
                        factor = u_buf[wave, table[0, a, tile], part].astype(jnp.float32)
                        rows.append(jnp.where(rank_ids < table[1, a, tile], factor, 0.0))
                    flipped = jnp.concatenate(rows, axis=0).T.astype(jnp.bfloat16)
                    lines = pl.ds(part * tile_rows, tile_rows)
                    if j == 0:
                        u_turn[chunk, wave, lines, 0:4 * rank_rows] = flipped
                    else:
                        u_give[chunk, wave, lines, :] = flipped
        send_turn(chunk).start()

    def served_here(tile):
        return (tile != partner_corner) & ~((tile == corner_of(across)) & serves_side(across))

    def use_tile(place, tile, wave):
        @pl.when(served_here(tile))
        def _():
            if wave == 0:
                send_v(place).wait_recv()
            serve(place, tile, wave, functools.partial(send_served, place))

        project(0, place, tile, place, wave)

    def at_end(level):
        return (level == 0) | (level == depth - 1)

    def forward(step, tile, wave):
        level = level_of(step)
        arrive(wave, tile)

        @pl.when(leaps & (tile == corner_of(across)))
        def _():
            leap(wave).start()

        @pl.when((level < z) & has_up)
        def _():
            along_z(wave, tile, 1).start()

        @pl.when((level > z) & has_down)
        def _():
            along_z(wave, tile, -1).start()

        held = wave == waves - 1

        crosses = ~(is_feeder & (step == depth - 2)) if held else step > 0

        @pl.when(crosses & ~(doubled & at_end(level)))
        def _():
            along_x(wave, tile).start()

        if held:
            @pl.when(is_feeder & (step == depth - 1))
            def _():
                along_x(wave, tile_at(0, 2 * step - 2)).start()

    def take_side(place, wave):
        tile = tile_at(0, place)
        arrive(wave, tile)
        share_edge(wave, tile)
        level = level_of(place // 2)
        passes = doubled & at_end(level)

        @pl.when(passes & (level <= z) & has_up)
        def _():
            along_z(wave, tile, 1).start()

        @pl.when(passes & (level >= z) & has_down)
        def _():
            along_z(wave, tile, -1).start()

        @pl.when((tile == partner_corner) & ~(doubled & at_wrap(partner)))
        def _():
            along_y(wave, tile).start()

    corner_place = 1
    for step in range(depth):
        corner_place += jnp.where(row_of(level_of(step), 1 - y, 1 - x) == corner, 2 * step, 0)

    def use_corner():
        for wave in range(waves):
            arrive(wave, corner)
            share_edge(wave, corner)

            @pl.when(serves_side(r))
            def _():
                if wave == 0:
                    send_v_side(0).wait_recv()
                serve(places, corner, wave, functools.partial(send_served_side, corner_place - 1))

            project(1, corner_place, corner, places, wave)

    def far_chunk(chunk, wave):
        right = coef[chunk, wave].reshape(-1, coef.shape[-1])
        return jnp.dot(u_turn[chunk, wave], right, preferred_element_type=jnp.float32)

    def place_of(offset):
        across_chip = jnp.where(offset == 1 - 2 * c, 2, 3)
        return jnp.where(offset % 2 == 0, jnp.where(offset == 2 * (beside - r), 0, 1), across_chip)

    def near_sum(wave):
        value = None
        for n in range(near_buf.shape[1]):
            left = near_buf[wave, n].reshape(2 * tile_rows, tile_rows)
            block = close[wave, place_of(offset_ref[0, n])] if n else tiles[wave, r]
            prod = jnp.dot(left, block, preferred_element_type=jnp.float32)
            value = prod if value is None else value + prod
        return value

    def await_chunk(chunk):
        await_bytes(u_give.at[0], t_recv.at[chunk])
        part = coef.at[chunk]
        if chunk < half:
            await_bytes(part.at[:, 1], g_recv.at[chunk])
        else:
            sem = s_recv.at[chunk - half]
            holds_corner = corner_place // 4 == chunk - half

            @pl.when(holds_corner)
            def _():
                await_bytes(part.at[:, :, 0:3], sem)
                await_bytes(give.at[0], g_recv.at[half])

            @pl.when(~holds_corner)
            def _():
                await_bytes(part, sem)

    def add_chunk(chunk):
        await_chunk(chunk)
        for wave in range(waves):
            total[wave] += far_chunk(chunk, wave)

    def await_near():
        for wave in range(waves):
            arrive(wave, own_slot)
            arrive(wave, edge_slot)
            close[wave, 0] = tiles[wave, beside]
            close[wave, 1] = tiles[wave, corner]

    def await_first():
        for chunk in range(half - 1):
            await_chunk(chunk)

    def first_sum(with_near, wave, carry):
        value = near_sum(wave) if with_near else jnp.zeros(total.shape[1:], jnp.float32)
        for chunk in range(half - 1):
            value += far_chunk(chunk, wave)
        total[wave] = value
        return carry

    def add_near(wave, carry):
        total[wave] += near_sum(wave)
        return carry

    def comes_early(step):
        return doubled & has_up & has_down & at_end(level_of(step))

    def spread(distance, carry):
        behind = 2 * distance - 1

        @pl.when(distance < depth)
        def _():
            place_u(distance)

        @pl.when(distance == 0)
        def _():
            for wave in range(waves):
                use_tile(0, r, wave)

        @pl.when((distance == depth) & serves_side(r))
        def _():
            use_corner()

        @pl.when(distance > 0)
        def _():
            for wave in range(waves):
                for sign in (1, -1):
                    level = z + sign * distance

                    @pl.when((level >= 0) & (level < depth))
                    def _():
                        first = 2 * distance - (1 if sign == 1 else 0)
                        step = jnp.where(distance <= middle, first, middle + distance)
                        tile = row_of(level, y, x)
                        forward(step, tile, wave)
                        use_tile(2 * step, tile, wave)

                if wave == waves - 1:
                    @pl.when(is_end & (distance == depth - 1))
                    def _():
                        for early in range(waves):
                            take_side(places - 1, early)

                @pl.when(~comes_early(distance - 1))
                def _():
                    @pl.when(~(is_end & (distance == depth)))
                    def _():
                        take_side(behind, wave)

                    use_tile(behind, tile_at(0, behind), wave)

                @pl.when(comes_early(distance) & (distance < depth))
                def _():
                    take_side(behind + 2, wave)
                    use_tile(behind + 2, tile_at(0, behind + 2), wave)

        return carry

    lax.fori_loop(0, depth + 1, spread, 0)

    @pl.when(~at_wrap(r) & ~serves_side(r))
    def _():
        use_corner()

    @pl.when(~at_wrap(r))
    def _():
        await_near()
        await_first()
        lax.fori_loop(0, waves, functools.partial(first_sum, True), 0)

    @pl.when(at_wrap(r))
    def _():
        await_first()
        lax.fori_loop(0, waves, functools.partial(first_sum, False), 0)

    add_chunk(half - 1)
    for chunk in range(half, depth - 1):
        add_chunk(chunk)

    @pl.when(at_wrap(r))
    def _():
        use_corner()
        await_near()
        lax.fori_loop(0, waves, add_near, 0)

    await_chunk(depth - 1)
    for wave in range(waves):
        value = total[wave] + far_chunk(depth - 1, wave)
        out_ref[wave] = combine_parts(value[:tile_rows], value[tile_rows:]).astype(out_ref.dtype)

    def await_count(parts, count, most, sem):
        for n in range(1, most + 1):
            @pl.when(count == n)
            def _():
                await_bytes(parts(n), sem)

    def one_if(flag):
        return jnp.where(flag, 1, 0)

    def some_tiles(n):
        return tiles.at[:, 0:n]

    def ends_but(level):
        return one_if(doubled) * (2 - one_if(at_end(level)))

    await_bytes(some_tiles(2), pair_sem.at[0])
    await_bytes(v_out.at[0:places - 1], v_send.at[0])
    await_bytes(give, g_send.at[0])
    await_bytes(u_give, t_send.at[0])
    sides = places - 1 - one_if(serves_side(across)) + one_if(serves_side(r))
    await_count(lambda n: served.at[0:n], sides, places, s_send.at[0])
    ups = one_if(has_up) * (z + 1 + one_if(doubled))
    await_count(some_tiles, ups, depth, send_sem.at[UP])
    downs = one_if(has_down) * (depth - z + one_if(doubled))
    await_count(some_tiles, downs, depth, send_sem.at[DOWN])
    await_count(some_tiles, depth - ends_but(z), depth, send_sem.at[ALONG_X])
    lines = one_if(leaps) + one_if(~(doubled & at_wrap(partner)))
    await_count(some_tiles, lines, 2, send_sem.at[ALONG_Y])


def fused_shards(incident, near_tiles, near_offsets, far_row, far_col, far_rank, far_count, far_u, far_v):
    waves, tile_rows, columns = incident.shape
    row_count, row_blocks = lax.axis_size("row"), lax.axis_size("col")
    slots, rank_rows = far_u.shape[3], far_u.shape[5]
    near_slots = near_tiles.shape[2]
    depth, places, half = row_count // 4, row_count // 2, row_count // 8
    bf16, f32 = jnp.bfloat16, jnp.float32
    any_space = pl.BlockSpec(memory_space=pl.ANY)
    dma = pltpu.SemaphoreType.DMA
    return pl.pallas_call(
        functools.partial(fused_kernel, depth),
        out_shape=pltpu.VMEM(incident.shape, bf16),
        in_specs=[any_space] * 9,
        out_specs=pl.BlockSpec(memory_space=pltpu.VMEM),
        scratch_shapes=[
            pltpu.VMEM((waves, row_count, tile_rows, columns), bf16),
            pltpu.VMEM((waves, 4, tile_rows, columns), bf16),
            pltpu.VMEM((waves, near_slots, 2, tile_rows, tile_rows), bf16),
            pltpu.VMEM((waves, slots, 2, rank_rows, tile_rows), bf16),
            pltpu.VMEM((waves, slots, 2, rank_rows, tile_rows), bf16),
            pltpu.VMEM((depth, waves, 2 * tile_rows, 8 * rank_rows), bf16),
            pltpu.VMEM((depth, waves, 2 * tile_rows, 4 * rank_rows), bf16),
            pltpu.VMEM((depth, waves, row_blocks, 4, rank_rows, columns), bf16),
            pltpu.VMEM((places + 1, waves, rank_rows, columns), bf16),
            pltpu.VMEM((places, waves, row_blocks, 2, rank_rows, tile_rows), bf16),
            pltpu.VMEM((places + 1, waves, row_blocks, 2, rank_rows, tile_rows), bf16),
            pltpu.VMEM((places + 1, waves, row_blocks, rank_rows, columns), bf16),
            pltpu.VMEM((waves, 2 * tile_rows, columns), f32),
            pltpu.SMEM(near_offsets.shape, jnp.int32),
            pltpu.SMEM(far_row.shape, jnp.int32),
            pltpu.SMEM(far_col.shape, jnp.int32),
            pltpu.SMEM(far_rank.shape, jnp.int32),
            pltpu.SMEM(far_count.shape, jnp.int32),
            pltpu.SMEM((slots,), jnp.int32),
            pltpu.SMEM((2, row_blocks, row_count), jnp.int32),
            dma((waves, row_count + 2)),
            dma((4,)),
            dma((1,)),
            dma((1,)),
            dma((places + 1,)),
            dma((1,)),
            dma((half,)),
            dma((1,)),
            dma((half + 1,)),
            dma((1,)),
            dma((depth,)),
            dma((8 + waves,)),
        ],
        compiler_params=pltpu.CompilerParams(collective_id=0, has_side_effects=True),
    )(near_offsets, far_row, far_col, far_rank, far_count, incident, near_tiles, far_u, far_v)


def solution(mesh):
    in_specs = (
        P(None, ("row", "col"), None),
        P(("row", "col"), None, None, None, None, None),
        P(("row", "col"), None),
        P("row", "col", None),
        P("row", "col", None),
        P("row", "col", None),
        P("row", "col"),
        P("row", "col", None, None, None, None, None),
        P("row", "col", None, None, None, None, None),
    )
    out_specs = P(None, ("row", "col"), None)
    paired = mesh.shape["col"] == 2 and mesh.shape["row"] % 8 == 0
    shards = fused_shards if paired else generic_shards
    return jax.shard_map(shards, mesh=mesh, in_specs=in_specs, out_specs=out_specs, check_vma=False)
```

```python
import functools

import jax
import jax.numpy as jnp
from jax import lax
from jax.experimental import pallas as pl
from jax.experimental.pallas import tpu as pltpu
from jax.sharding import PartitionSpec as P

MESH = pl.DeviceIdType.MESH
UP, DOWN, ALONG_Y, ALONG_X = range(4)


def from_behind(value, axis, steps):
    count = lax.axis_size(axis)
    pairs = [(source, (source + steps) % count) for source in range(count)]
    return lax.ppermute(value, axis, pairs)


def combine_parts(real_prod, imag_prod):
    half_width = real_prod.shape[-1] // 2
    return jnp.concatenate(
        [
            real_prod[..., :half_width] - imag_prod[..., half_width:],
            real_prod[..., half_width:] + imag_prod[..., :half_width],
        ],
        axis=-1,
    )


def far_partial(
    wave_tiles,
    rows_local,
    cols_local,
    rank_local,
    live_count,
    u_wave,
    v_wave,
    group_limit,
    row_blocks,
):
    group_size = 16
    tile_rows = wave_tiles.shape[1]
    columns = wave_tiles.shape[2]
    rank_size = v_wave.shape[2]
    slot_ids = jnp.arange(group_size, dtype=jnp.int32)
    rank_ids = jnp.arange(rank_size, dtype=jnp.int32)

    def add_group(group_step, far_sum):
        first_slot = group_step * group_size
        rows_group = lax.dynamic_slice_in_dim(rows_local, first_slot, group_size)
        cols_group = lax.dynamic_slice_in_dim(cols_local, first_slot, group_size)
        rank_group = lax.dynamic_slice_in_dim(rank_local, first_slot, group_size)
        v_group = lax.dynamic_slice_in_dim(v_wave, first_slot, group_size, 0)
        u_group = lax.dynamic_slice_in_dim(u_wave, first_slot, group_size, 0)
        slot_tiles = jnp.take(wave_tiles, cols_group, axis=0)
        real_prod = jnp.einsum(
            "fkq,fqc->fkc", v_group[:, 0], slot_tiles, preferred_element_type=jnp.float32
        )
        imag_prod = jnp.einsum(
            "fkq,fqc->fkc", v_group[:, 1], slot_tiles, preferred_element_type=jnp.float32
        )
        live_mask = (first_slot + slot_ids < live_count)[:, None] & (
            rank_ids[None, :] < rank_group[:, None]
        )
        coefficients = (
            combine_parts(real_prod, imag_prod) * live_mask[:, :, None].astype(jnp.float32)
        ).astype(jnp.bfloat16)
        real_back = jnp.einsum(
            "fkp,fkc->fpc", u_group[:, 0], coefficients, preferred_element_type=jnp.float32
        )
        imag_back = jnp.einsum(
            "fkp,fkc->fpc", u_group[:, 1], coefficients, preferred_element_type=jnp.float32
        )
        contrib = combine_parts(real_back, imag_back)
        return far_sum.at[rows_group].add(contrib)

    zero_sum = jnp.zeros((row_blocks, tile_rows, columns), jnp.float32)
    return lax.fori_loop(0, group_limit, add_group, zero_sum)


def reduce_rows(far_sum, row_blocks, tile_rows, columns):
    flat_rows = far_sum.reshape(row_blocks * tile_rows, columns)
    return lax.psum_scatter(flat_rows, "col", scatter_dimension=0, tiled=True)


def generic_shards(incident, near_tiles, near_offsets, far_row, far_col, far_rank, far_count, far_u, far_v):
    wave_count, tile_rows, columns = incident.shape
    row_blocks = lax.axis_size("col")
    slot_count = far_row.shape[2]
    stacked = []
    for shift_by in (2, 1, 0, -1, -2):
        if shift_by == 0:
            stacked.append(incident)
        else:
            stacked.append(from_behind(incident, ("row", "col"), shift_by))
    neighbour = jnp.stack(stacked, axis=1)
    near_inputs = jnp.take(neighbour, near_offsets[0] + 2, axis=1)
    local_near = near_tiles[0]
    real_prod = jnp.einsum(
        "wnpq,wnqc->wpc", local_near[:, :, 0], near_inputs, preferred_element_type=jnp.float32
    )
    imag_prod = jnp.einsum(
        "wnpq,wnqc->wpc", local_near[:, :, 1], near_inputs, preferred_element_type=jnp.float32
    )
    near_total = combine_parts(real_prod, imag_prod)
    rows_local = far_row[0, 0]
    cols_local = far_col[0, 0]
    rank_local = far_rank[0, 0]
    live_count = far_count[0, 0]
    group_limit = slot_count // 16
    gathered = lax.all_gather(incident, "row", axis=1, tiled=True)
    outputs = []
    for wave_index in range(wave_count):
        wave_columns = gathered[wave_index]
        wave_tiles = wave_columns.reshape(-1, tile_rows, columns)
        far_sum = far_partial(
            wave_tiles,
            rows_local,
            cols_local,
            rank_local,
            live_count,
            far_u[0, 0, wave_index],
            far_v[0, 0, wave_index],
            group_limit,
            row_blocks,
        )
        own_rows = reduce_rows(far_sum, row_blocks, tile_rows, columns)
        outputs.append(near_total[wave_index] + own_rows)
    return jnp.stack(outputs, axis=0).astype(jnp.bfloat16)


def fused_kernel(
    depth, offset_hbm, row_hbm, col_hbm, rank_hbm, count_hbm, x_hbm, near_hbm, u_hbm, v_hbm, out_ref,
    tiles, close, near_buf, u_buf, v_buf, u_turn, u_give, coef, give, v_out, v_in, served, total, offset_ref, row_ref, col_ref, rank_ref, count_ref, keys, table,
    recv_sem, send_sem, pair_sem, v_send, v_recv, s_send, s_recv, g_send, g_recv, t_send, t_recv, load_sem,
):
    waves = tiles.shape[0]
    row_count = depth * 4
    places = depth * 2
    half = depth // 2
    row_blocks = table.shape[1]
    slots = v_buf.shape[1]
    rank_rows = v_buf.shape[3]
    tile_rows = tiles.shape[2]
    r = lax.axis_index("row")
    c = lax.axis_index("col")
    z, y, x = r // 4, (r // 2) % 2, r % 2
    own_slot, edge_slot = row_count, row_count + 1
    edge_tile = (r + 1 - 2 * c + row_count) % row_count
    partner = r + 2 * (1 - 2 * y)
    has_up, has_down = z < depth - 1, z > 0
    beside = r + 1 - 2 * x
    low_end, high_end = 2, row_count - 3
    doubled = c == 1
    is_end = ((r == low_end) | (r == high_end)) & ~doubled
    is_feeder = ((beside == low_end) | (beside == high_end)) & ~doubled
    across = partner + 1 - 2 * x

    def corner_of(row):
        return (row + 2 * (row % 2) - 1 + row_count) % row_count

    def at_wrap(row):
        return (row == 0) | (row == row_count - 1)

    leaps = doubled & at_wrap(across)
    leapt = doubled & at_wrap(r)

    def serves_side(row):
        from_end = jnp.minimum(row, row_count - 1 - row)
        return (from_end == 1) | (from_end > 3)

    corner, partner_corner = corner_of(r), corner_of(partner)

    def row_of(tz, ty, tx):
        return (tz * 2 + ty) * 2 + tx

    load_x = [
        pltpu.make_async_copy(x_hbm.at[wave], tiles.at[wave, r], load_sem.at[3 + wave])
        for wave in range(waves)
    ]
    load_v = pltpu.make_async_copy(v_hbm.at[0, 0], v_buf, load_sem.at[0])
    load_u = pltpu.make_async_copy(u_hbm.at[0, 0], u_buf, load_sem.at[1])
    load_near = pltpu.make_async_copy(near_hbm.at[0], near_buf, load_sem.at[2])
    small = (
        (row_hbm, row_ref), (col_hbm, col_ref), (rank_hbm, rank_ref),
        (count_hbm, count_ref), (offset_hbm, offset_ref),
    )
    load_small = [
        pltpu.make_async_copy(source, target, load_sem.at[3 + waves + n])
        for n, (source, target) in enumerate(small)
    ]
    for load in load_small + load_x + [load_v, load_u, load_near]:
        load.start()

    barrier = pltpu.get_barrier_semaphore()

    def greet(device):
        pl.semaphore_signal(barrier, inc=1, device_id=device, device_id_type=MESH)

    for device in ((partner, c), (partner, 1 - c), (beside, c), (beside, 1 - c), (r, 1 - c)):
        greet(device)

    @pl.when(leapt)
    def _():
        greet((across, c))

    @pl.when(has_up)
    def _():
        greet((row_of(z + 1, y, x), c))

    @pl.when(has_down)
    def _():
        greet((row_of(z - 1, y, x), c))

    for load in load_small:
        load.wait()
    for s in range(slots):
        key = row_ref[0, 0, s] * row_count + col_ref[0, 0, s]
        keys[s] = jnp.where(s < count_ref[0, 0], key, -1)

    def look_up(a, tile):
        wanted = a * row_count + tile
        slot, rank = jnp.int32(0), jnp.int32(0)
        for s in range(slots):
            hit = keys[s] == wanted
            slot = jnp.where(hit, s, slot)
            rank = jnp.where(hit, rank_ref[0, 0, s], rank)
        table[0, a, tile] = slot
        table[1, a, tile] = rank

    pl.semaphore_wait(barrier, 5 + jnp.where(has_up, 1, 0) + jnp.where(has_down, 1, 0) + jnp.where(leaps, 1, 0))

    def copy_to(source, target, sent, received, device):
        return pltpu.make_async_remote_copy(
            src_ref=source,
            dst_ref=target,
            send_sem=sent,
            recv_sem=received,
            device_id=device,
            device_id_type=MESH,
        )

    def hop(wave, tile, link, row):
        here = tiles.at[wave, tile]
        return copy_to(here, here, send_sem.at[link], recv_sem.at[wave, tile], (row, c))

    def along_z(wave, tile, step):
        return hop(wave, tile, (1 - step) // 2, row_of(z + step, y, x))

    def along_x(wave, tile):
        return hop(wave, tile, ALONG_X, beside)

    def along_y(wave, tile):
        return hop(wave, tile, ALONG_Y, partner)

    def leap(wave):
        return hop(wave, corner_of(across), ALONG_Y, across)

    def to_pair(wave, tile, slot):
        return copy_to(
            tiles.at[wave, tile],
            close.at[wave, slot - row_count + 2],
            pair_sem.at[0],
            recv_sem.at[wave, slot],
            (r, 1 - c),
        )

    def send_v(place):
        return copy_to(
            v_out.at[place], v_in.at[place], v_send.at[0], v_recv.at[place], (partner, c)
        )

    def send_v_side(place):
        return copy_to(
            v_out.at[place], v_in.at[places], v_send.at[0], v_recv.at[places], (beside, c)
        )

    def send_served(place, wave, j):
        return copy_to(
            served.at[place, wave, j],
            coef.at[half + place // 4, wave, j, place % 4],
            s_send.at[0],
            s_recv.at[place // 4],
            (partner, c if j == 0 else 1 - c),
        )

    def send_served_side(place, wave, j):
        return copy_to(
            served.at[places, wave, j],
            coef.at[half + place // 4, wave, j, place % 4],
            s_send.at[0],
            s_recv.at[place // 4],
            (beside, c if j == 0 else 1 - c),
        )

    def send_give(plane, place, index):
        return copy_to(
            give.at[index],
            coef.at[plane * half + place // 4, :, 1, place % 4],
            g_send.at[0],
            g_recv.at[half if plane else place // 4],
            (r, 1 - c),
        )

    def send_turn(chunk):
        return copy_to(
            u_give.at[chunk],
            u_turn.at[chunk, :, :, pl.ds(4 * rank_rows, 4 * rank_rows)],
            t_send.at[0],
            t_recv.at[chunk],
            (r, 1 - c),
        )

    middle = jnp.minimum(z, depth - 1 - z)

    def level_of(step):
        reach = (step + 1) // 2
        near_level = z + jnp.where(step % 2 == 1, reach, -reach)
        beyond = step - middle
        far_level = z + jnp.where(depth - 1 - z > z, beyond, -beyond)
        return jnp.where(step <= 2 * middle, near_level, far_level)

    def tile_at(plane, place):
        level, other = level_of(place // 2), place % 2
        return row_of(level, y + plane - 2 * y * plane, x + other - 2 * x * other)

    def complex_rows(prod, at):
        at = 2 * rank_rows * at
        return combine_parts(prod[at:at + rank_rows], prod[at + rank_rows:at + 2 * rank_rows])

    def project(plane, place, tile, index, wave):
        factors = [v_buf[wave, table[0, a, tile]].reshape(2 * rank_rows, -1) for a in (c, 1 - c)]
        prod = jnp.dot(
            jnp.concatenate(factors, axis=0), tiles[wave, tile], preferred_element_type=jnp.float32
        )
        chunk = plane * half + place // 4
        coef[chunk, wave, 0, place % 4] = complex_rows(prod, 0).astype(jnp.bfloat16)
        give[index, wave] = complex_rows(prod, 1).astype(jnp.bfloat16)
        if wave == waves - 1:
            send_give(plane, place, index).start()

    def serve(place, tile, wave, send):
        left = v_in[place, wave].reshape(row_blocks * 2 * rank_rows, -1)
        prod = jnp.dot(left, tiles[wave, tile], preferred_element_type=jnp.float32)
        for j in range(row_blocks):
            served[place, wave, j] = complex_rows(prod, j).astype(jnp.bfloat16)
        for j in range(row_blocks):
            send(wave, j).start()

    def await_bytes(part, sem):
        pltpu.make_async_copy(part, part, sem).wait()

    def arrive(wave, tile):
        await_bytes(tiles.at[wave, r], recv_sem.at[wave, tile])

    def share_edge(wave, tile):
        @pl.when(tile == edge_tile)
        def _():
            to_pair(wave, tile, edge_slot).start()

    for wave in range(waves):
        load_x[wave].wait()
        along_x(wave, r).start()

        @pl.when(has_up)
        def _():
            along_z(wave, r, 1).start()

        @pl.when(has_down)
        def _():
            along_z(wave, r, -1).start()

        to_pair(wave, r, own_slot).start()

    load_v.wait()

    def push_v(place, carry):
        tile = tile_at(1, place)
        for a in range(row_blocks):
            look_up(a, tile)

        @pl.when(tile != corner)
        def _():
            for wave in range(waves):
                for j, a in enumerate((c, 1 - c)):
                    v_out[place, wave, j] = v_buf[wave, table[0, a, tile]]
            aside = (tile == corner_of(beside)) & serves_side(beside)

            @pl.when(aside)
            def _():
                send_v_side(place).start()

            @pl.when(~aside)
            def _():
                send_v(place).start()

        return carry

    lax.fori_loop(0, places, push_v, 0)

    def find_own(place, carry):
        for a in range(row_blocks):
            look_up(a, tile_at(0, place))
        return carry

    lax.fori_loop(0, places, find_own, 0)
    load_u.wait()
    load_near.wait()
    rank_ids = lax.broadcasted_iota(jnp.int32, (rank_rows, tile_rows), 0)

    def place_u(chunk):
        plane, first = chunk // half, (chunk % half) * 4
        for wave in range(waves):
            for j, a in enumerate((c, 1 - c)):
                for part in range(2):
                    rows = []
                    for at in range(4):
                        tile = tile_at(plane, first + at)
                        factor = u_buf[wave, table[0, a, tile], part].astype(jnp.float32)
                        rows.append(jnp.where(rank_ids < table[1, a, tile], factor, 0.0))
                    flipped = jnp.concatenate(rows, axis=0).T.astype(jnp.bfloat16)
                    lines = pl.ds(part * tile_rows, tile_rows)
                    if j == 0:
                        u_turn[chunk, wave, lines, 0:4 * rank_rows] = flipped
                    else:
                        u_give[chunk, wave, lines, :] = flipped
        send_turn(chunk).start()

    def served_here(tile):
        return (tile != partner_corner) & ~((tile == corner_of(across)) & serves_side(across))

    def use_tile(place, tile, wave):
        @pl.when(served_here(tile))
        def _():
            if wave == 0:
                send_v(place).wait_recv()
            serve(place, tile, wave, functools.partial(send_served, place))

        project(0, place, tile, place, wave)

    def at_end(level):
        return (level == 0) | (level == depth - 1)

    def forward(step, tile, wave):
        level = level_of(step)
        arrive(wave, tile)

        @pl.when(leaps & (tile == corner_of(across)))
        def _():
            leap(wave).start()

        @pl.when((level < z) & has_up)
        def _():
            along_z(wave, tile, 1).start()

        @pl.when((level > z) & has_down)
        def _():
            along_z(wave, tile, -1).start()

        held = wave == waves - 1

        crosses = ~(is_feeder & (step == depth - 2)) if held else step > 0

        @pl.when(crosses & ~(doubled & at_end(level)))
        def _():
            along_x(wave, tile).start()

        if held:
            @pl.when(is_feeder & (step == depth - 1))
            def _():
                along_x(wave, tile_at(0, 2 * step - 2)).start()

    def take_side(place, wave):
        tile = tile_at(0, place)
        arrive(wave, tile)
        share_edge(wave, tile)
        level = level_of(place // 2)
        passes = doubled & at_end(level)

        @pl.when(passes & (level <= z) & has_up)
        def _():
            along_z(wave, tile, 1).start()

        @pl.when(passes & (level >= z) & has_down)
        def _():
            along_z(wave, tile, -1).start()

        @pl.when((tile == partner_corner) & ~(doubled & at_wrap(partner)))
        def _():
            along_y(wave, tile).start()

    corner_place = 1
    for step in range(depth):
        corner_place += jnp.where(row_of(level_of(step), 1 - y, 1 - x) == corner, 2 * step, 0)

    def use_corner():
        for wave in range(waves):
            arrive(wave, corner)
            share_edge(wave, corner)

            @pl.when(serves_side(r))
            def _():
                if wave == 0:
                    send_v_side(0).wait_recv()
                serve(places, corner, wave, functools.partial(send_served_side, corner_place - 1))

            project(1, corner_place, corner, places, wave)

    def far_chunk(chunk, wave):
        right = coef[chunk, wave].reshape(-1, coef.shape[-1])
        return jnp.dot(u_turn[chunk, wave], right, preferred_element_type=jnp.float32)

    def place_of(offset):
        across_chip = jnp.where(offset == 1 - 2 * c, 2, 3)
        return jnp.where(offset % 2 == 0, jnp.where(offset == 2 * (beside - r), 0, 1), across_chip)

    def near_sum(wave, slots_used):
        value = None
        for n in slots_used:
            left = near_buf[wave, n].reshape(2 * tile_rows, tile_rows)
            block = close[wave, place_of(offset_ref[0, n])] if n else tiles[wave, r]
            prod = jnp.dot(left, block, preferred_element_type=jnp.float32)
            value = prod if value is None else value + prod
        return value

    def await_chunk(chunk):
        await_bytes(u_give.at[0], t_recv.at[chunk])
        part = coef.at[chunk]
        if chunk < half:
            await_bytes(part.at[:, 1], g_recv.at[chunk])
        else:
            sem = s_recv.at[chunk - half]
            holds_corner = corner_place // 4 == chunk - half

            @pl.when(holds_corner)
            def _():
                await_bytes(part.at[:, :, 0:3], sem)
                await_bytes(give.at[0], g_recv.at[half])

            @pl.when(~holds_corner)
            def _():
                await_bytes(part, sem)

    def add_chunk(chunk):
        await_chunk(chunk)
        for wave in range(waves):
            total[wave] += far_chunk(chunk, wave)

    def await_near():
        for wave in range(waves):
            arrive(wave, own_slot)
            arrive(wave, edge_slot)
            close[wave, 0] = tiles[wave, beside]
            close[wave, 1] = tiles[wave, corner]

    def await_first():
        for chunk in range(half - 1):
            await_chunk(chunk)

    def first_sum(with_near, wave, carry):
        value = near_sum(wave, range(near_buf.shape[1]) if with_near else (0,))
        for chunk in range(half - 1):
            value += far_chunk(chunk, wave)
        total[wave] = value
        return carry

    def add_near(wave, carry):
        total[wave] += near_sum(wave, range(1, near_buf.shape[1]))
        return carry

    def comes_early(step):
        return doubled & has_up & has_down & at_end(level_of(step))

    def spread(distance, carry):
        behind = 2 * distance - 1

        @pl.when(distance < depth)
        def _():
            place_u(distance)

        @pl.when(distance == 0)
        def _():
            for wave in range(waves):
                use_tile(0, r, wave)

        @pl.when((distance == depth) & serves_side(r))
        def _():
            use_corner()

        @pl.when(distance > 0)
        def _():
            for wave in range(waves):
                for sign in (1, -1):
                    level = z + sign * distance

                    @pl.when((level >= 0) & (level < depth))
                    def _():
                        first = 2 * distance - (1 if sign == 1 else 0)
                        step = jnp.where(distance <= middle, first, middle + distance)
                        tile = row_of(level, y, x)
                        forward(step, tile, wave)
                        use_tile(2 * step, tile, wave)

                if wave == waves - 1:
                    @pl.when(is_end & (distance == depth - 1))
                    def _():
                        for early in range(waves):
                            take_side(places - 1, early)

                @pl.when(~comes_early(distance - 1))
                def _():
                    @pl.when(~(is_end & (distance == depth)))
                    def _():
                        take_side(behind, wave)

                    use_tile(behind, tile_at(0, behind), wave)

                @pl.when(comes_early(distance) & (distance < depth))
                def _():
                    take_side(behind + 2, wave)
                    use_tile(behind + 2, tile_at(0, behind + 2), wave)

        return carry

    lax.fori_loop(0, depth + 1, spread, 0)

    @pl.when(~at_wrap(r) & ~serves_side(r))
    def _():
        use_corner()

    @pl.when(~at_wrap(r))
    def _():
        await_near()
        await_first()
        lax.fori_loop(0, waves, functools.partial(first_sum, True), 0)

    @pl.when(at_wrap(r))
    def _():
        await_first()
        lax.fori_loop(0, waves, functools.partial(first_sum, False), 0)

    add_chunk(half - 1)
    for chunk in range(half, depth - 1):
        add_chunk(chunk)

    @pl.when(at_wrap(r))
    def _():
        use_corner()
        await_near()
        lax.fori_loop(0, waves, add_near, 0)

    await_chunk(depth - 1)
    for wave in range(waves):
        value = total[wave] + far_chunk(depth - 1, wave)
        out_ref[wave] = combine_parts(value[:tile_rows], value[tile_rows:]).astype(out_ref.dtype)

    def await_count(parts, count, most, sem):
        for n in range(1, most + 1):
            @pl.when(count == n)
            def _():
                await_bytes(parts(n), sem)

    def one_if(flag):
        return jnp.where(flag, 1, 0)

    def some_tiles(n):
        return tiles.at[:, 0:n]

    def ends_but(level):
        return one_if(doubled) * (2 - one_if(at_end(level)))

    await_bytes(some_tiles(2), pair_sem.at[0])
    await_bytes(v_out.at[0:places - 1], v_send.at[0])
    await_bytes(give, g_send.at[0])
    await_bytes(u_give, t_send.at[0])
    sides = places - 1 - one_if(serves_side(across)) + one_if(serves_side(r))
    await_count(lambda n: served.at[0:n], sides, places, s_send.at[0])
    ups = one_if(has_up) * (z + 1 + one_if(doubled))
    await_count(some_tiles, ups, depth, send_sem.at[UP])
    downs = one_if(has_down) * (depth - z + one_if(doubled))
    await_count(some_tiles, downs, depth, send_sem.at[DOWN])
    await_count(some_tiles, depth - ends_but(z), depth, send_sem.at[ALONG_X])
    lines = one_if(leaps) + one_if(~(doubled & at_wrap(partner)))
    await_count(some_tiles, lines, 2, send_sem.at[ALONG_Y])


def fused_shards(incident, near_tiles, near_offsets, far_row, far_col, far_rank, far_count, far_u, far_v):
    waves, tile_rows, columns = incident.shape
    row_count, row_blocks = lax.axis_size("row"), lax.axis_size("col")
    slots, rank_rows = far_u.shape[3], far_u.shape[5]
    near_slots = near_tiles.shape[2]
    depth, places, half = row_count // 4, row_count // 2, row_count // 8
    bf16, f32 = jnp.bfloat16, jnp.float32
    any_space = pl.BlockSpec(memory_space=pl.ANY)
    dma = pltpu.SemaphoreType.DMA
    return pl.pallas_call(
        functools.partial(fused_kernel, depth),
        out_shape=pltpu.VMEM(incident.shape, bf16),
        in_specs=[any_space] * 9,
        out_specs=pl.BlockSpec(memory_space=pltpu.VMEM),
        scratch_shapes=[
            pltpu.VMEM((waves, row_count, tile_rows, columns), bf16),
            pltpu.VMEM((waves, 4, tile_rows, columns), bf16),
            pltpu.VMEM((waves, near_slots, 2, tile_rows, tile_rows), bf16),
            pltpu.VMEM((waves, slots, 2, rank_rows, tile_rows), bf16),
            pltpu.VMEM((waves, slots, 2, rank_rows, tile_rows), bf16),
            pltpu.VMEM((depth, waves, 2 * tile_rows, 8 * rank_rows), bf16),
            pltpu.VMEM((depth, waves, 2 * tile_rows, 4 * rank_rows), bf16),
            pltpu.VMEM((depth, waves, row_blocks, 4, rank_rows, columns), bf16),
            pltpu.VMEM((places + 1, waves, rank_rows, columns), bf16),
            pltpu.VMEM((places, waves, row_blocks, 2, rank_rows, tile_rows), bf16),
            pltpu.VMEM((places + 1, waves, row_blocks, 2, rank_rows, tile_rows), bf16),
            pltpu.VMEM((places + 1, waves, row_blocks, rank_rows, columns), bf16),
            pltpu.VMEM((waves, 2 * tile_rows, columns), f32),
            pltpu.SMEM(near_offsets.shape, jnp.int32),
            pltpu.SMEM(far_row.shape, jnp.int32),
            pltpu.SMEM(far_col.shape, jnp.int32),
            pltpu.SMEM(far_rank.shape, jnp.int32),
            pltpu.SMEM(far_count.shape, jnp.int32),
            pltpu.SMEM((slots,), jnp.int32),
            pltpu.SMEM((2, row_blocks, row_count), jnp.int32),
            dma((waves, row_count + 2)),
            dma((4,)),
            dma((1,)),
            dma((1,)),
            dma((places + 1,)),
            dma((1,)),
            dma((half,)),
            dma((1,)),
            dma((half + 1,)),
            dma((1,)),
            dma((depth,)),
            dma((8 + waves,)),
        ],
        compiler_params=pltpu.CompilerParams(collective_id=0, has_side_effects=True),
    )(near_offsets, far_row, far_col, far_rank, far_count, incident, near_tiles, far_u, far_v)


def solution(mesh):
    in_specs = (
        P(None, ("row", "col"), None),
        P(("row", "col"), None, None, None, None, None),
        P(("row", "col"), None),
        P("row", "col", None),
        P("row", "col", None),
        P("row", "col", None),
        P("row", "col"),
        P("row", "col", None, None, None, None, None),
        P("row", "col", None, None, None, None, None),
    )
    out_specs = P(None, ("row", "col"), None)
    paired = mesh.shape["col"] == 2 and mesh.shape["row"] % 8 == 0
    shards = fused_shards if paired else generic_shards
    return jax.shard_map(shards, mesh=mesh, in_specs=in_specs, out_specs=out_specs, check_vma=False)
```
